8 devices in a mesh: dp: 1 (over z), ffn: 2 (over y), emb: 4 (over x, core).
Axes of the slice: x: 2, y: 2, z: 1, core: 2. Of those that a mesh axis runs over, the one named last changes fastest.
Arguments:
- hidden: bfloat16 [4096, 1024], P('dp', 'emb')
- norm_pre: bfloat16 [1024], P('emb')
- norm_post: bfloat16 [1024], P('emb')
- w_router: bfloat16 [1024, 32], P('emb')
- w_gate: bfloat16 [32, 1024, 512], P(None, 'emb', 'ffn')
- w_up: bfloat16 [32, 1024, 512], P(None, 'emb', 'ffn')
- w_down: bfloat16 [32, 512, 1024], P(None, 'ffn', 'emb')
- choice: int32 [4096, 8], P('dp')
Outputs:
- output: bfloat16 [4096, 1024], P('dp', 'emb')
All inputs are finite; a program needn't handle non-finite values.
Results may differ from the reference program's by a relative error of at most 0.0125918.
Values are sent between devices in bfloat16 or wider.
A program may use at most 1 GiB of HBM per device.

```python
import math
import jax
import jax.numpy as jnp
from jax import lax

D = 1024
E = 32
F = 512
TOP = 8
B = 4096
CAP = 2 * B * TOP // E
EPS = 1e-5


def width_profile(key, size):
    slope = jax.random.uniform(key, (), minval=1.5, maxval=2.5)
    return jnp.exp(slope * (jnp.arange(size, dtype=jnp.float32) / size - 0.5))


def draw_choice(key):
    key_hot, key_perm, key_score = jax.random.split(key, 3)
    hot_id = jax.random.randint(key_hot, (), 0, E)
    forced = jax.random.permutation(key_perm, B) < (3 * B) // 4
    expert_ids = jnp.arange(E)
    score = jax.random.randint(key_score, (B, E), 1, 1048576) * E + expert_ids[None, :]
    score = jnp.where(forced[:, None] & (expert_ids[None, :] == hot_id), 0, score)
    return jnp.argsort(score, axis=1, stable=True)[:, :TOP].astype(jnp.int32)


def setup_inputs(seed: int = 0, part: int = 0) -> dict:
    base_key = jax.random.key(seed)
    part_keys = jax.random.split(jax.random.fold_in(base_key, part), 4)
    shared_keys = jax.random.split(base_key, 7)
    row_scale = jnp.exp(0.5 * jax.random.normal(part_keys[0], (B, 1)))
    hidden = jax.random.normal(part_keys[1], (B, D)) * row_scale * width_profile(part_keys[2], D)[None, :]
    norm_pre = 1.0 + 0.3 * jax.random.normal(shared_keys[0], (D,))
    norm_post = 1.0 + 0.3 * jax.random.normal(shared_keys[1], (D,))
    w_router = jax.random.normal(shared_keys[2], (D, E)) * (1.5 / math.sqrt(D))
    w_gate = jax.random.normal(shared_keys[3], (E, D, F)) * (1.0 / math.sqrt(D))
    w_up = jax.random.normal(shared_keys[4], (E, D, F)) * (1.0 / math.sqrt(D))
    w_down = jax.random.normal(shared_keys[5], (E, F, D)) * (1.0 / math.sqrt(F)) * width_profile(shared_keys[6], D)[None, None, :]
    return {
        'hidden': hidden.astype(jnp.bfloat16),
        'norm_pre': norm_pre.astype(jnp.bfloat16),
        'norm_post': norm_post.astype(jnp.bfloat16),
        'w_router': w_router.astype(jnp.bfloat16),
        'w_gate': w_gate.astype(jnp.bfloat16),
        'w_up': w_up.astype(jnp.bfloat16),
        'w_down': w_down.astype(jnp.bfloat16),
        'choice': draw_choice(part_keys[3]),
    }


def route_tokens(choice, router_prob):
    onehot = (choice[:, :, None] == jnp.arange(E)[None, None, :]).astype(jnp.int32)
    assigned = jnp.sum(onehot, axis=1)
    before = jnp.cumsum(assigned, axis=0) - assigned
    slot_idx = jnp.sum(onehot * before[:, None, :], axis=2)
    position = jnp.where(slot_idx < CAP, choice * CAP + slot_idx, E * CAP)
    gate_val = jnp.take_along_axis(router_prob, choice, axis=1)
    flat_pos = position.reshape(-1)
    token_ids = jnp.repeat(jnp.arange(B, dtype=jnp.int32), TOP)
    slot_token = jnp.full((E * CAP,), B, jnp.int32).at[flat_pos].set(token_ids, mode='drop')
    slot_gate = jnp.zeros((E * CAP,), jnp.float32).at[flat_pos].set(gate_val.reshape(-1), mode='drop')
    return position, slot_token, slot_gate


def expert_ffn(operands):
    slot_rows, gate_w, up_w, down_w = operands
    z_gate = jnp.dot(slot_rows, gate_w, preferred_element_type=jnp.float32).astype(jnp.bfloat16)
    z_up = jnp.dot(slot_rows, up_w, preferred_element_type=jnp.float32).astype(jnp.bfloat16)
    act_val = (jax.nn.gelu(z_gate.astype(jnp.float32), approximate=True) * z_up.astype(jnp.float32)).astype(jnp.bfloat16)
    return jnp.dot(act_val, down_w, preferred_element_type=jnp.float32).astype(jnp.bfloat16)


def reference(hidden, norm_pre, norm_post, w_router, w_gate, w_up, w_down, choice):
    hid_f32 = hidden.astype(jnp.float32)
    inv_pre = lax.rsqrt(jnp.mean(hid_f32 * hid_f32, axis=1, keepdims=True) + EPS)
    normed = (hid_f32 * inv_pre * norm_pre.astype(jnp.float32)).astype(jnp.bfloat16)
    logits = jnp.dot(normed, w_router, preferred_element_type=jnp.float32)
    router_prob = jax.nn.softmax(logits, axis=1)
    position, slot_token, slot_gate = route_tokens(choice, router_prob)
    expert_in = jnp.take(normed, slot_token, axis=0, mode='fill', fill_value=0).reshape(E, CAP, D)
    expert_out = lax.map(expert_ffn, (expert_in, w_gate, w_up, w_down))
    weighted = (expert_out.reshape(E * CAP, D).astype(jnp.float32) * slot_gate[:, None]).astype(jnp.bfloat16)
    picked = jnp.take(weighted, position, axis=0, mode='fill', fill_value=0)
    mix_sum = jnp.sum(picked.astype(jnp.float32), axis=1)
    inv_post = lax.rsqrt(jnp.mean(mix_sum * mix_sum, axis=1, keepdims=True) + EPS)
    return (hid_f32 + mix_sum * inv_post * norm_post.astype(jnp.float32)).astype(jnp.bfloat16)
```

```python
import functools
import math

import jax
import jax.numpy as jnp
from jax import lax
from jax.experimental import pallas as pl
from jax.experimental.pallas import tpu as pltpu
from jax.sharding import PartitionSpec as P

EPS = 1e-5
LANES = 128
MESH = pl.DeviceIdType.MESH


def gelu_tanh(z):
    return z * (0.5 * (1.0 + jnp.tanh(math.sqrt(2.0 / math.pi) * (z + 0.044715 * (z * z * z)))))


def kernel(
    experts, capacity,
    h_ref, wg_ref, wu_ref, wd_ref, small_ref, choice_ref, out_ref,
    hb, sm, w0, w1, w2, xn, gates, acc, rbuf, ob, gb,
    h_send, h_recv, s_send, s_recv, w_send, w_recv, w_own, f_send, f_recv, r_send, r_recv, o_send, o_recv,
):
    num_tok, lw = h_ref.shape
    fw = wg_ref.shape[2]
    half = num_tok // 2
    quarter = num_tok // 8
    local_e = experts // 4
    tile = 256
    bf16, f32 = jnp.bfloat16, jnp.float32

    f = lax.axis_index("ffn")
    i = lax.axis_index("emb")
    x, c = i // 2, i % 2
    q = 2 * x + f
    sib = 2 * x + (1 - c)

    def chip(d):
        x2 = (x + d // 2) % 2
        f2 = (f + d % 2) % 2
        return x2, f2, 2 * x2 + f2

    def rows(start, size):
        return pl.ds(pl.multiple_of(start, 128), size)

    barrier = pltpu.get_barrier_semaphore()
    for df in range(2):
        for di in range(4):
            if df or di:
                pl.semaphore_signal(
                    barrier, inc=1, device_id={"ffn": (f + df) % 2, "emb": (i + di) % 4}, device_id_type=MESH
                )
    pl.semaphore_wait(barrier, 7)

    def remote(src, dst, send, recv, f2, i2):
        return pltpu.make_async_remote_copy(
            src_ref=src, dst_ref=dst, send_sem=send, recv_sem=recv,
            device_id={"ffn": f2, "emb": i2}, device_id_type=MESH,
        )

    def await_bytes(ref, sem):
        pltpu.make_async_copy(ref, ref, sem).wait()

    own_h = pltpu.make_async_copy(h_ref.at[rows(c * half, half), :], hb.at[i], h_recv.at[i])
    own_s = pltpu.make_async_copy(small_ref, sm.at[i], s_recv.at[i])
    own_h.start()
    own_s.start()
    peers = [(sib, 1 - c)] + [(2 * (1 - x) + c2, c2) for c2 in range(2)]
    for n, (i2, c2) in enumerate(peers):
        remote(small_ref, sm.at[i], s_send.at[n], s_recv.at[i], f, i2).start()
        remote(h_ref.at[rows(c2 * half, half), :], hb.at[i], h_send.at[n], h_recv.at[i], f, i2).start()

    def blocks(j, fs, es):
        return (
            w0.at[j, fs, rows(es * lw, lw), :],
            w1.at[j, fs, rows(es * lw, lw), :],
            w2.at[j, es, rows(fs * fw, fw), :],
        )

    def group(j):
        return w0.at[j, 0, pl.ds(0, 3 * lw), :]

    def send_expert(j):
        dst = blocks(j, f, i)
        e = local_e * q + j
        for src, to in zip((wg_ref.at[e], wu_ref.at[e], wd_ref.at[e]), dst):
            pltpu.make_async_copy(src, to, w_own.at[j]).start()
            remote(src, to, f_send.at[j, 0], f_recv.at[j, 0], f, sib).start()
        for d in (3, 2, 1):
            x2, f2, q2 = chip(d)
            e2 = local_e * q2 + j
            for src, to in zip((wg_ref.at[e2], wu_ref.at[e2], wd_ref.at[e2]), dst):
                remote(src, to, w_send.at[j, d - 1], w_recv.at[j, d - 1], f2, 2 * x2 + c).start()

    ahead = 4
    for j in range(ahead):
        send_expert(j)

    lane = lax.broadcasted_iota(jnp.int32, (tile, LANES), 1)

    def chosen(start):
        ch = choice_ref[rows(start, tile), :]
        a = jnp.zeros((tile, LANES), f32)
        for k in range(choice_ref.shape[1]):
            a = a + jnp.where(ch[:, k : k + 1] == lane, 1.0, 0.0)
        return a

    def count(n, total):
        return total + jnp.sum(chosen(n * tile), axis=0, keepdims=True)

    first = lax.fori_loop(0, half // tile, count, jnp.zeros((1, LANES), f32))
    strict = lax.broadcasted_iota(jnp.int32, (tile, tile), 0) > lax.broadcasted_iota(jnp.int32, (tile, tile), 1)
    strict = jnp.where(strict, 1.0, 0.0).astype(bf16)

    def place(n, carry):
        a = chosen(c * half + n * tile)
        before = carry + jnp.dot(strict, a.astype(bf16), preferred_element_type=f32)
        gates[rows(n * tile, tile), :] = jnp.where(before < capacity, a, 0.0)
        acc[rows(n * tile, tile), :] = jnp.zeros((tile, acc.shape[1]), f32)
        return carry + jnp.sum(a, axis=0, keepdims=True)

    lax.fori_loop(0, half // tile, place, first * c.astype(f32))

    for b in range(4):
        await_bytes(sm.at[b], s_recv.at[b])
        await_bytes(hb.at[b], h_recv.at[b])

    def route(n, _):
        r = rows(n * tile, tile)
        sq = jnp.zeros((tile, 1), f32)
        for b in range(4):
            hv = hb[b, r, :].astype(f32)
            sq = sq + jnp.sum(hv * hv, axis=1, keepdims=True)
        inv = lax.rsqrt(sq / (4 * lw) + EPS)
        logits = jnp.zeros((tile, LANES), f32)
        for b in range(4):
            normed = (hb[b, r, :].astype(f32) * inv * sm[b, LANES : LANES + 1, :].astype(f32)).astype(bf16)
            xn[r, b * lw : (b + 1) * lw] = normed
            logits = logits + lax.dot_general(
                normed, sm[b, 0:LANES, :], (((1,), (1,)), ((), ())), preferred_element_type=f32
            )
        logits = jnp.where(lane < experts, logits, -jnp.inf)
        p = jnp.exp(logits - jnp.max(logits, axis=1, keepdims=True))
        p = p / jnp.sum(p, axis=1, keepdims=True)
        gates[r, :] = jnp.where(gates[r, :] > 0.0, p, 0.0)
        return 0

    lax.fori_loop(0, half // tile, route, 0)

    lane_q = lax.broadcasted_iota(jnp.int32, (quarter, LANES), 1)

    def expert(j, _):
        @pl.when(j + ahead < local_e)
        def _():
            send_expert(j + ahead)

        await_bytes(group(j), w_own.at[j])
        for d in (1, 2, 3):
            x2, f2, _q2 = chip(d)
            await_bytes(group(j), w_recv.at[j, d - 1])
            for ref in blocks(j, f2, 2 * x2 + c):
                remote(ref, ref, f_send.at[j, d], f_recv.at[j, d], f, sib).start()
        for d in range(4):
            await_bytes(group(j), f_recv.at[j, d])

        def step(n, _):
            d = (n + 1) % 4
            x2, f2, q2 = chip(d)
            r = rows(q2 * quarter, quarter)
            gate = jnp.sum(jnp.where(lane_q == local_e * q + j, gates[r, :], 0.0), axis=1, keepdims=True)
            for s in range(2):
                z0 = jnp.dot(xn[r, :], w0[j, s], preferred_element_type=f32).astype(bf16).astype(f32)
                z1 = jnp.dot(xn[r, :], w1[j, s], preferred_element_type=f32).astype(bf16).astype(f32)
                g = jnp.where(gate > 0.0, gelu_tanh(z0) * z1, 0.0)
                gb[:, s * fw : (s + 1) * fw] = g.astype(bf16)
            for b in range(4):
                y = jnp.dot(gb[...], w2[j, b], preferred_element_type=f32).astype(bf16).astype(f32)
                u = (y * gate).astype(bf16).astype(f32)
                acc[r, b * lw : (b + 1) * lw] += u

            @pl.when((j == local_e - 1) & (d > 0))
            def _():
                remote(
                    acc.at[r, :], rbuf.at[d - 1], r_send.at[d - 1], r_recv.at[d - 1], f2, 2 * x2 + c
                ).start()

            return 0

        lax.fori_loop(0, 4, step, 0)
        return 0

    lax.fori_loop(0, local_e, expert, 0)

    for d in (1, 2, 3):
        await_bytes(rbuf.at[d - 1], r_recv.at[d - 1])
    part = 128

    def finish(n, _):
        r = rows(q * quarter + n * part, part)
        s = rows(n * part, part)
        m = []
        sq = jnp.zeros((part, 1), f32)
        for b in range(4):
            cols = slice(b * lw, (b + 1) * lw)
            v = (acc[r, cols] + rbuf[0, s, cols]) + (rbuf[1, s, cols] + rbuf[2, s, cols])
            sq = sq + jnp.sum(v * v, axis=1, keepdims=True)
            m.append(v)
        inv = lax.rsqrt(sq / (4 * lw) + EPS)
        for b in range(4):
            post = sm[b, LANES + 1 : LANES + 2, :].astype(f32)
            ob[b, s, :] = (hb[b, r, :].astype(f32) + m[b] * inv * post).astype(bf16)
        return 0

    lax.fori_loop(0, quarter // part, finish, 0)

    mine = out_ref.at[rows(c * half + q * quarter, quarter), :]
    me = 4 * f + i
    for df in range(2):
        for di in range(4):
            f2, i2 = (f + df) % 2, (i + di) % 4
            if df or di:
                remote(ob.at[i2], mine, o_send.at[4 * df + di], o_recv.at[me], f2, i2).start()
            else:
                pltpu.make_async_copy(ob.at[i], mine, o_send.at[0]).start()
    for df in range(2):
        for di in range(4):
            if df or di:
                await_bytes(ob.at[0], o_recv.at[4 * ((f + df) % 2) + (i + di) % 4])
            await_bytes(ob.at[0], o_send.at[4 * df + di])

    for n in range(3):
        await_bytes(sm.at[0], s_send.at[n])
        await_bytes(hb.at[0], h_send.at[n])
        await_bytes(rbuf.at[0], r_send.at[n])

    def drain(j, _):
        for d in range(4):
            await_bytes(group(j), f_send.at[j, d])
            if d:
                await_bytes(group(j), w_send.at[j, d - 1])
        return 0

    lax.fori_loop(0, local_e, drain, 0)


def solution(mesh):
    emb_size = mesh.shape["emb"]
    ffn_size = mesh.shape["ffn"]
    assert emb_size == 4 and ffn_size == 2

    def local_block(hidden, norm_pre, norm_post, w_router, w_gate, w_up, w_down, choice):
        num_tok, lw = hidden.shape
        experts, _, fw = w_gate.shape
        top_k = choice.shape[1]
        capacity = 2 * num_tok * top_k // experts
        width, ffn = lw * emb_size, fw * ffn_size
        half, quarter, local_e = num_tok // 2, num_tok // 8, experts // 4
        small_rows = LANES + 16
        small = jnp.concatenate([
            jnp.pad(w_router.T, ((0, LANES - experts), (0, 0))),
            norm_pre[None, :],
            norm_post[None, :],
            jnp.zeros((14, lw), jnp.bfloat16),
        ])
        bf16, f32 = jnp.bfloat16, jnp.float32
        dma = pltpu.SemaphoreType.DMA
        anywhere = pl.BlockSpec(memory_space=pl.ANY)
        flops = 2 * 3 * half * local_e * width * ffn
        return pl.pallas_call(
            functools.partial(kernel, experts, capacity),
            out_shape=jax.ShapeDtypeStruct((num_tok, lw), bf16),
            in_specs=[anywhere] * 5 + [pl.BlockSpec(memory_space=pltpu.VMEM)],
            out_specs=anywhere,
            scratch_shapes=[
                pltpu.VMEM((4, half, lw), bf16),
                pltpu.VMEM((4, small_rows, lw), bf16),
                pltpu.VMEM((local_e, 2, width, fw), bf16),
                pltpu.VMEM((local_e, 2, width, fw), bf16),
                pltpu.VMEM((local_e, 4, ffn, lw), bf16),
                pltpu.VMEM((half, width), bf16),
                pltpu.VMEM((half, LANES), f32),
                pltpu.VMEM((half, width), f32),
                pltpu.VMEM((3, quarter, width), f32),
                pltpu.VMEM((4, quarter, lw), bf16),
                pltpu.VMEM((quarter, ffn), bf16),
                dma((3,)), dma((4,)), dma((3,)), dma((4,)),
                dma((local_e, 3)), dma((local_e, 3)), dma((local_e,)),
                dma((local_e, 4)), dma((local_e, 4)),
                dma((3,)), dma((3,)), dma((8,)), dma((8,)),
            ],
            compiler_params=pltpu.CompilerParams(
                collective_id=0, has_side_effects=True, vmem_limit_bytes=67043328
            ),
            cost_estimate=pl.CostEstimate(flops=flops, bytes_accessed=60 << 20, transcendentals=half * local_e * ffn),
        )(hidden, w_gate, w_up, w_down, small, choice)

    in_specs = (P('dp', 'emb'), P('emb'), P('emb'), P('emb', None), P(None, 'emb', 'ffn'), P(None, 'emb', 'ffn'), P(None, 'ffn', 'emb'), P('dp', None))
    return jax.shard_map(local_block, mesh=mesh, in_specs=in_specs, out_specs=P('dp', 'emb'), check_vma=False)
```

```python
import functools
import math

import jax
import jax.numpy as jnp
from jax import lax
from jax.experimental import pallas as pl
from jax.experimental.pallas import tpu as pltpu
from jax.sharding import PartitionSpec as P

EPS = 1e-5
LANES = 128
MESH = pl.DeviceIdType.MESH


def gelu_tanh(z):
    return z * (0.5 * (1.0 + jnp.tanh(math.sqrt(2.0 / math.pi) * (z + 0.044715 * (z * z * z)))))


def kernel(
    experts, capacity,
    h_ref, wg_ref, wu_ref, wd_ref, small_ref, choice_ref, out_ref,
    hb, sm, w0, w1, w2, xn, gates, acc, ybuf, xbuf, ob, gb,
    h_send, h_recv, hf_send, hf_recv, s_send, s_recv, w_send, w_recv, w_own, f_send, f_recv,
    y_send, y_recv, x_send, x_recv, o_send, o_recv,
):
    num_tok, lw = h_ref.shape
    fw = wg_ref.shape[2]
    half = num_tok // 2
    quarter = num_tok // 8
    local_e = experts // 4
    tile = 256
    parts = y_recv.shape[1]
    part = quarter // parts
    cut = ybuf.shape[2]
    bf16, f32 = jnp.bfloat16, jnp.float32

    f = lax.axis_index("ffn")
    i = lax.axis_index("emb")
    x, c = i // 2, i % 2
    q = 2 * x + f
    sib = 2 * x + (1 - c)

    def chip(d):
        x2 = (x + d // 2) % 2
        f2 = (f + d % 2) % 2
        return x2, f2, 2 * x2 + f2

    def rows(start, size):
        return pl.ds(pl.multiple_of(start, 128), size)

    barrier = pltpu.get_barrier_semaphore()
    for df in range(2):
        for di in range(4):
            if df or di:
                pl.semaphore_signal(
                    barrier, inc=1, device_id={"ffn": (f + df) % 2, "emb": (i + di) % 4}, device_id_type=MESH
                )
    pl.semaphore_wait(barrier, 7)

    def remote(src, dst, send, recv, f2, i2):
        return pltpu.make_async_remote_copy(
            src_ref=src, dst_ref=dst, send_sem=send, recv_sem=recv,
            device_id={"ffn": f2, "emb": i2}, device_id_type=MESH,
        )

    def await_bytes(ref, sem):
        pltpu.make_async_copy(ref, ref, sem).wait()

    own_h = pltpu.make_async_copy(h_ref.at[rows(c * half, half), :], hb.at[i], h_recv.at[i])
    own_s = pltpu.make_async_copy(small_ref, sm.at[i], s_recv.at[i])
    own_h.start()
    own_s.start()
    across = rows(f * (half // 2), half // 2)
    far = rows((1 - f) * (half // 2), half // 2)
    for c2 in range(2):
        i2 = 2 * (1 - x) + c2
        remote(small_ref, sm.at[i], s_send.at[c2], s_recv.at[i], f, i2).start()
        src = h_ref.at[rows(c2 * half + f * (half // 2), half // 2), :]
        remote(src, hb.at[i, across, :], h_send.at[c2], h_recv.at[i], f, i2).start()
    remote(small_ref, sm.at[i], s_send.at[2], s_recv.at[i], f, sib).start()
    remote(h_ref.at[rows((1 - c) * half, half), :], hb.at[i], h_send.at[2], h_recv.at[i], f, sib).start()

    def blocks(j, fs, es):
        return (
            w0.at[j, fs, rows(es * lw, lw), :],
            w1.at[j, fs, rows(es * lw, lw), :],
            w2.at[j, es, rows(fs * fw, fw), :],
        )

    def group(j):
        return w0.at[j, 0, pl.ds(0, 3 * lw), :]

    def send_expert(j):
        dst = blocks(j, f, i)
        e = local_e * q + j
        for src, to in zip((wg_ref.at[e], wu_ref.at[e], wd_ref.at[e]), dst):
            pltpu.make_async_copy(src, to, w_own.at[j]).start()
            remote(src, to, f_send.at[j, 0], f_recv.at[j, 0], f, sib).start()
        for d in (3, 2, 1):
            x2, f2, q2 = chip(d)
            e2 = local_e * q2 + j
            for src, to in zip((wg_ref.at[e2], wu_ref.at[e2], wd_ref.at[e2]), dst):
                remote(src, to, w_send.at[j, d - 1], w_recv.at[j, d - 1], f2, 2 * x2 + c).start()

    ahead = 4
    for j in range(2):
        send_expert(j)

    sublane = lax.broadcasted_iota(jnp.int32, (experts, tile), 0)

    def chosen(start):
        ch = choice_ref[:, pl.ds(pl.multiple_of(start, LANES), tile)]
        a = jnp.zeros((experts, tile), f32)
        for k in range(choice_ref.shape[0]):
            a = a + jnp.where(ch[k : k + 1, :] == sublane, 1.0, 0.0)
        return a

    def count(n, total):
        return total + jnp.sum(chosen(n * tile), axis=1, keepdims=True)

    first = lax.fori_loop(0, half // tile, count, jnp.zeros((experts, 1), f32))
    strict = lax.broadcasted_iota(jnp.int32, (tile, tile), 0) < lax.broadcasted_iota(jnp.int32, (tile, tile), 1)
    strict = jnp.where(strict, 1.0, 0.0).astype(bf16)

    def place(n, carry):
        a = chosen(c * half + n * tile)
        before = carry + jnp.dot(a.astype(bf16), strict, preferred_element_type=f32)
        gates[rows(n * tile, tile), :] = jnp.where(before < capacity, a, 0.0).T
        acc[rows(n * tile, tile), :] = jnp.zeros((tile, acc.shape[1]), f32)
        return carry + jnp.sum(a, axis=1, keepdims=True)

    lax.fori_loop(0, half // tile, place, first * c.astype(f32))

    for c2 in range(2):
        e2 = 2 * (1 - x) + c2
        await_bytes(hb.at[e2, across, :], h_recv.at[e2])
        ref = hb.at[e2, across, :]
        remote(ref, ref, hf_send.at[c2], hf_recv.at[c2], 1 - f, i).start()
    for j in range(2, ahead):
        send_expert(j)
    for c2 in range(2):
        await_bytes(hb.at[2 * x + c2], h_recv.at[2 * x + c2])
        await_bytes(hb.at[2 * (1 - x) + c2, far, :], hf_recv.at[c2])
    for b in range(4):
        await_bytes(sm.at[b], s_recv.at[b])

    def route(n, _):
        r = rows(n * tile, tile)
        sq = jnp.zeros((tile, 1), f32)
        for b in range(4):
            hv = hb[b, r, :].astype(f32)
            sq = sq + jnp.sum(hv * hv, axis=1, keepdims=True)
        inv = lax.rsqrt(sq / (4 * lw) + EPS)
        logits = jnp.zeros((tile, experts), f32)
        for b in range(4):
            normed = (hb[b, r, :].astype(f32) * inv * sm[b, experts : experts + 1, :].astype(f32)).astype(bf16)
            xn[r, b * lw : (b + 1) * lw] = normed
            logits = logits + lax.dot_general(
                normed, sm[b, 0:experts, :], (((1,), (1,)), ((), ())), preferred_element_type=f32
            )
        p = jnp.exp(logits - jnp.max(logits, axis=1, keepdims=True))
        p = p / jnp.sum(p, axis=1, keepdims=True)
        gates[r, :] = jnp.where(gates[r, :] > 0.0, p, 0.0)
        return 0

    lax.fori_loop(0, half // tile, route, 0)

    def to_y(src, slot, t):
        return remote(
            src, ybuf.at[slot, rows(t * part, part), :], y_send.at[slot, t], y_recv.at[slot, t], 1 - f, i
        )

    def to_x(src, slot, t):
        return remote(
            src, xbuf.at[slot, rows(t * part, part), :], x_send.at[slot, t], x_recv.at[slot, t], f, 2 * (1 - x) + c
        )

    def y_to_x(src, t):
        return remote(
            src, ybuf.at[2, rows(t * part, part), :], y_send.at[2, t], y_recv.at[2, t], f, 2 * (1 - x) + c
        )

    def x_to_y(src, t):
        return remote(src, xbuf.at[2, rows(t * part, part), :], x_send.at[2, t], x_recv.at[2, t], 1 - f, i)

    def out_rows(xs, fs, cs, t):
        return rows(cs * half + (2 * xs + fs) * quarter + t * part, part)

    lane_q = lax.broadcasted_iota(jnp.int32, (quarter, experts), 1)

    def expert(j, _):
        @pl.when(j + ahead < local_e)
        def _():
            send_expert(j + ahead)

        await_bytes(group(j), w_own.at[j])
        for d in (1, 2, 3):
            x2, f2, _q2 = chip(d)
            await_bytes(group(j), w_recv.at[j, d - 1])
            for ref in blocks(j, f2, 2 * x2 + c):
                remote(ref, ref, f_send.at[j, d], f_recv.at[j, d], f, sib).start()
        for d in range(4):
            await_bytes(group(j), f_recv.at[j, d])

        def step(n, _):
            x2 = (x + n + 1) % 2
            f2 = (f + 1 - n // 2) % 2
            r = rows((2 * x2 + f2) * quarter, quarter)
            gate = jnp.sum(jnp.where(lane_q == local_e * q + j, gates[r, :], 0.0), axis=1, keepdims=True)
            for s in range(2):
                z0 = jnp.dot(xn[r, :], w0[j, s], preferred_element_type=f32).astype(bf16).astype(f32)
                z1 = jnp.dot(xn[r, :], w1[j, s], preferred_element_type=f32).astype(bf16).astype(f32)
                g = jnp.where(gate > 0.0, gelu_tanh(z0) * z1, 0.0)
                gb[:, s * fw : (s + 1) * fw] = g.astype(bf16)
            for b in range(4):
                y = jnp.dot(gb[...], w2[j, b], preferred_element_type=f32).astype(bf16).astype(f32)
                u = (y * gate).astype(bf16).astype(f32)
                acc[r, b * lw : (b + 1) * lw] += u

            start = (2 * x2 + f2) * quarter

            @pl.when((j == local_e - 1) & (n < 2))
            def _():
                for t in range(parts):
                    src = acc.at[rows(start + t * part, part), 0:cut]
                    to_y(src, n, t).start()

            @pl.when((j == local_e - 1) & (n % 2 == 0) & (n < 3))
            def _():
                for t in range(parts):
                    src = acc.at[rows(start + t * part, part), cut:]
                    to_x(src, n // 2, t).start()

            return 0

        lax.fori_loop(0, 4, step, 0)
        return 0

    lax.fori_loop(0, local_e, expert, 0)

    def mid(t, _):
        xr = rows((2 * (1 - x) + f) * quarter + t * part, part)
        yr = rows((2 * x + 1 - f) * quarter + t * part, part)
        buf = rows(t * part, part)
        await_bytes(xbuf.at[0, buf, :], x_recv.at[0, t])
        acc[yr, cut:] = acc[yr, cut:] + xbuf[0, buf, :]
        x_to_y(acc.at[yr, cut:], t).start()
        await_bytes(ybuf.at[0, buf, :], y_recv.at[0, t])
        acc[xr, 0:cut] = acc[xr, 0:cut] + ybuf[0, buf, :]
        y_to_x(acc.at[xr, 0:cut], t).start()
        return 0

    lax.fori_loop(0, parts, mid, 0)

    step_rows = 128

    def finish(t, _):
        buf = rows(t * part, part)
        for n in (1, 2):
            await_bytes(ybuf.at[n, buf, :], y_recv.at[n, t])
            await_bytes(xbuf.at[n, buf, :], x_recv.at[n, t])

        def norm(n, _):
            r = rows(q * quarter + t * part + n * step_rows, step_rows)
            s = rows(t * part + n * step_rows, step_rows)
            lo = acc[r, 0:cut] + (ybuf[1, s, :] + ybuf[2, s, :])
            hi = acc[r, cut:] + (xbuf[1, s, :] + xbuf[2, s, :])
            sq = jnp.sum(lo * lo, axis=1, keepdims=True) + jnp.sum(hi * hi, axis=1, keepdims=True)
            inv = lax.rsqrt(sq / (4 * lw) + EPS)
            acc[r, 0:cut] = lo * inv
            acc[r, cut:] = hi * inv
            for b in range(4):
                post = sm[b, experts + 1 : experts + 2, :].astype(f32)
                ob[b, s, :] = (hb[b, r, :].astype(f32) + acc[r, b * lw : (b + 1) * lw] * post).astype(bf16)
            return 0

        lax.fori_loop(0, part // step_rows, norm, 0)

        mine = out_ref.at[out_rows(x, f, c, t), :]
        for c2 in range(2):
            i2 = 2 * (1 - x) + c2
            remote(ob.at[i2, buf, :], mine, o_send.at[2 + c2, t], o_recv.at[1 + c, t], f, i2).start()
        for c2 in range(2):
            i2 = 2 * x + c2
            remote(ob.at[i2, buf, :], mine, o_send.at[4 + c2, t], o_recv.at[3 + c, t], 1 - f, i2).start()
        pltpu.make_async_copy(ob.at[i, buf, :], mine, o_send.at[0, t]).start()
        remote(ob.at[sib, buf, :], mine, o_send.at[1, t], o_recv.at[0, t], f, sib).start()
        return 0

    lax.fori_loop(0, parts, finish, 0)

    def pass_on(t, _):
        for c2 in range(2):
            there = out_ref.at[out_rows(1 - x, f, c2, t), :]
            await_bytes(there, o_recv.at[1 + c2, t])
            remote(there, there, o_send.at[6 + c2, t], o_recv.at[5 + c2, t], 1 - f, i).start()
        return 0

    lax.fori_loop(0, parts, pass_on, 0)

    def close(t, _):
        buf = rows(t * part, part)
        here = ob.at[0, buf, :]
        for n in (0, 3, 4, 5, 6):
            await_bytes(here, o_recv.at[n, t])
        for n in range(8):
            await_bytes(here, o_send.at[n, t])
        for n in range(3):
            await_bytes(ybuf.at[0, buf, :], y_send.at[n, t])
            await_bytes(xbuf.at[0, buf, :], x_send.at[n, t])
        return 0

    lax.fori_loop(0, parts, close, 0)
    for n in range(3):
        await_bytes(sm.at[0], s_send.at[n])
    await_bytes(hb.at[0], h_send.at[2])
    for n in range(2):
        await_bytes(hb.at[0, across, :], h_send.at[n])
        await_bytes(hb.at[0, across, :], hf_send.at[n])

    def drain(j, _):
        for d in range(4):
            await_bytes(group(j), f_send.at[j, d])
            if d:
                await_bytes(group(j), w_send.at[j, d - 1])
        return 0

    lax.fori_loop(0, local_e, drain, 0)


def solution(mesh):
    emb_size = mesh.shape["emb"]
    ffn_size = mesh.shape["ffn"]
    assert emb_size == 4 and ffn_size == 2

    def local_block(hidden, norm_pre, norm_post, w_router, w_gate, w_up, w_down, choice):
        num_tok, lw = hidden.shape
        experts, _, fw = w_gate.shape
        top_k = choice.shape[1]
        capacity = 2 * num_tok * top_k // experts
        width, ffn = lw * emb_size, fw * ffn_size
        half, quarter, local_e = num_tok // 2, num_tok // 8, experts // 4
        small_rows = experts + 16
        row = lax.broadcasted_iota(jnp.int32, (small_rows, lw), 0)
        norms = jnp.where(row == experts, norm_pre[None, :], norm_post[None, :])
        small = jnp.where(row < experts, jnp.pad(w_router.T, ((0, 16), (0, 0))), norms)
        parts, cut = 2, 384
        bf16, f32 = jnp.bfloat16, jnp.float32
        dma = pltpu.SemaphoreType.DMA
        anywhere = pl.BlockSpec(memory_space=pl.ANY)
        flops = 2 * 3 * half * local_e * width * ffn
        return pl.pallas_call(
            functools.partial(kernel, experts, capacity),
            out_shape=jax.ShapeDtypeStruct((num_tok, lw), bf16),
            in_specs=[anywhere] * 5 + [pl.BlockSpec(memory_space=pltpu.VMEM)],
            out_specs=anywhere,
            scratch_shapes=[
                pltpu.VMEM((4, half, lw), bf16),
                pltpu.VMEM((4, small_rows, lw), bf16),
                pltpu.VMEM((local_e, 2, width, fw), bf16),
                pltpu.VMEM((local_e, 2, width, fw), bf16),
                pltpu.VMEM((local_e, 4, ffn, lw), bf16),
                pltpu.VMEM((half, width), bf16),
                pltpu.VMEM((half, experts), f32),
                pltpu.VMEM((half, width), f32),
                pltpu.VMEM((3, quarter, cut), f32),
                pltpu.VMEM((3, quarter, width - cut), f32),
                pltpu.VMEM((4, quarter, lw), bf16),
                pltpu.VMEM((quarter, ffn), bf16),
                dma((3,)), dma((4,)), dma((2,)), dma((2,)), dma((3,)), dma((4,)),
                dma((local_e, 3)), dma((local_e, 3)), dma((local_e,)),
                dma((local_e, 4)), dma((local_e, 4)),
                dma((3, parts)), dma((3, parts)), dma((3, parts)), dma((3, parts)),
                dma((8, parts)), dma((7, parts)),
            ],
            compiler_params=pltpu.CompilerParams(
                collective_id=0, has_side_effects=True, vmem_limit_bytes=67043328
            ),
            cost_estimate=pl.CostEstimate(flops=flops, bytes_accessed=60 << 20, transcendentals=half * local_e * ffn),
        )(hidden, w_gate, w_up, w_down, small, choice.T)

    in_specs = (P('dp', 'emb'), P('emb'), P('emb'), P('emb', None), P(None, 'emb', 'ffn'), P(None, 'emb', 'ffn'), P(None, 'ffn', 'emb'), P('dp', None))
    return jax.shard_map(local_block, mesh=mesh, in_specs=in_specs, out_specs=P('dp', 'emb'), check_vma=False)
```

```python
import functools
import math

import jax
import jax.numpy as jnp
from jax import lax
from jax.experimental import pallas as pl
from jax.experimental.pallas import tpu as pltpu
from jax.sharding import PartitionSpec as P

EPS = 1e-5
LANES = 128
MESH = pl.DeviceIdType.MESH


PIECES = 8
Y_FIRST = (0, 2, 6)
ORDER = (
    "D3", "D1", "D2", "N2", "D4", "N5", "D6", "m2", "m3", "M2", "M3", "m1",
    "D5", "M1", "m4", "m6", "N3", "M4", "N1", "N6", "t2", "D0", "m5", "M6",
    "M5", "t3", "N0", "N4", "m0", "t1", "e2", "D7", "t5", "t6", "e3", "t4",
    "e1", "M0", "N7", "m7", "M7", "e4", "e5", "e6", "t0", "t7", "e0", "e7",
)


def plan():
    steps = [(p[0], int(p[1:])) for p in ORDER]
    head = next(n for n, p in enumerate(steps) if p[0] == "m")
    first, tile = [], 0
    for kind, t in steps[:head]:
        need = t // (PIECES // 2) + (2 if kind == "N" and t not in Y_FIRST else 0)
        tile = max(tile, need)
        first.append((kind, t, tile))
    return first, steps[head:]


FIRST, REST = plan()


def gelu_tanh(z):
    return z * (0.5 * (1.0 + jnp.tanh(math.sqrt(2.0 / math.pi) * (z + 0.044715 * (z * z * z)))))


def kernel(
    experts, capacity,
    h_ref, wg_ref, wu_ref, wd_ref, small_ref, choice_ref, out_ref,
    hb, sm, w0, w1, w2, xn, gates, acc, rbuf, sq_own, sq_far, ob, gb,
    h_send, h_recv, hf_send, hf_recv, s_send, s_recv, w_send, w_recv, w_own, f_send, f_recv,
    r_send, r_recv, q_send, q_recv, o_send, o_recv,
):
    num_tok, lw = h_ref.shape
    fw = wg_ref.shape[2]
    half = num_tok // 2
    quarter = num_tok // 8
    local_e = experts // 4
    tile = 256
    part = 128
    parts = quarter * 2 // part
    bf16, f32 = jnp.bfloat16, jnp.float32

    f = lax.axis_index("ffn")
    i = lax.axis_index("emb")
    x, c = i // 2, i % 2
    q = 2 * x + f
    sib = 2 * x + (1 - c)

    def chip(d):
        x2 = (x + d // 2) % 2
        f2 = (f + d % 2) % 2
        return x2, f2, 2 * x2 + f2

    def rows(start, size):
        return pl.ds(pl.multiple_of(start, 128), size)

    barrier = pltpu.get_barrier_semaphore()
    for df in range(2):
        for di in range(4):
            if df or di:
                pl.semaphore_signal(
                    barrier, inc=1, device_id={"ffn": (f + df) % 2, "emb": (i + di) % 4}, device_id_type=MESH
                )
    pl.semaphore_wait(barrier, 7)

    def remote(src, dst, send, recv, f2, i2):
        return pltpu.make_async_remote_copy(
            src_ref=src, dst_ref=dst, send_sem=send, recv_sem=recv,
            device_id={"ffn": f2, "emb": i2}, device_id_type=MESH,
        )

    def await_bytes(ref, sem):
        pltpu.make_async_copy(ref, ref, sem).wait()

    own_h = pltpu.make_async_copy(h_ref.at[rows(c * half, half), :], hb.at[i], h_recv.at[i])
    own_s = pltpu.make_async_copy(small_ref, sm.at[i], s_recv.at[i])
    own_h.start()
    own_s.start()
    across = rows(f * (half // 2), half // 2)
    far = rows((1 - f) * (half // 2), half // 2)
    for c2 in range(2):
        i2 = 2 * (1 - x) + c2
        remote(small_ref, sm.at[i], s_send.at[c2], s_recv.at[i], f, i2).start()
        src = h_ref.at[rows(c2 * half + f * (half // 2), half // 2), :]
        remote(src, hb.at[i, across, :], h_send.at[c2], h_recv.at[i], f, i2).start()
    remote(small_ref, sm.at[i], s_send.at[2], s_recv.at[i], f, sib).start()
    remote(h_ref.at[rows((1 - c) * half, half), :], hb.at[i], h_send.at[2], h_recv.at[i], f, sib).start()

    def blocks(j, fs, es):
        return (
            w0.at[j, fs, rows(es * lw, lw), :],
            w1.at[j, fs, rows(es * lw, lw), :],
            w2.at[j, es, rows(fs * fw, fw), :],
        )

    def group(j):
        return w0.at[j, 0, pl.ds(0, 3 * lw), :]

    def send_expert(j):
        dst = blocks(j, f, i)
        e = local_e * q + j
        for src, to in zip((wg_ref.at[e], wu_ref.at[e], wd_ref.at[e]), dst):
            pltpu.make_async_copy(src, to, w_own.at[j]).start()
            remote(src, to, f_send.at[j, 0], f_recv.at[j, 0], f, sib).start()
        for d in (3, 2, 1):
            x2, f2, q2 = chip(d)
            e2 = local_e * q2 + j
            for src, to in zip((wg_ref.at[e2], wu_ref.at[e2], wd_ref.at[e2]), dst):
                remote(src, to, w_send.at[j, d - 1], w_recv.at[j, d - 1], f2, 2 * x2 + c).start()

    ahead = 3
    for j in range(2):
        send_expert(j)

    sublane = lax.broadcasted_iota(jnp.int32, (experts, tile), 0)

    def chosen(start):
        ch = choice_ref[:, pl.ds(pl.multiple_of(start, LANES), tile)]
        a = jnp.zeros((experts, tile), f32)
        for k in range(choice_ref.shape[0]):
            a = a + jnp.where(ch[k : k + 1, :] == sublane, 1.0, 0.0)
        return a

    def count(n, total):
        return total + jnp.sum(chosen(n * tile), axis=1, keepdims=True)

    first = lax.fori_loop(0, half // tile, count, jnp.zeros((experts, 1), f32))
    strict = lax.broadcasted_iota(jnp.int32, (tile, tile), 0) < lax.broadcasted_iota(jnp.int32, (tile, tile), 1)
    strict = jnp.where(strict, 1.0, 0.0).astype(bf16)

    def place(n, carry):
        a = chosen(c * half + n * tile)
        before = carry + jnp.dot(a.astype(bf16), strict, preferred_element_type=f32)
        gates[rows(n * tile, tile), :] = jnp.where(before < capacity, a, 0.0).T
        for xs in range(2):
            acc[xs, rows(n * tile, tile), :] = jnp.zeros((tile, 2 * lw), f32)
        return carry + jnp.sum(a, axis=1, keepdims=True)

    lax.fori_loop(0, half // tile, place, first * c.astype(f32))

    for c2 in range(2):
        e2 = 2 * (1 - x) + c2
        await_bytes(hb.at[e2, across, :], h_recv.at[e2])
        ref = hb.at[e2, across, :]
        remote(ref, ref, hf_send.at[c2], hf_recv.at[c2], 1 - f, i).start()
    for j in range(2, ahead):
        send_expert(j)
    for c2 in range(2):
        await_bytes(hb.at[2 * x + c2], h_recv.at[2 * x + c2])
        await_bytes(hb.at[2 * (1 - x) + c2, far, :], hf_recv.at[c2])
    for b in range(4):
        await_bytes(sm.at[b], s_recv.at[b])

    def route(n, _):
        r = rows(n * tile, tile)
        sq = jnp.zeros((tile, 1), f32)
        for b in range(4):
            hv = hb[b, r, :].astype(f32)
            sq = sq + jnp.sum(hv * hv, axis=1, keepdims=True)
        inv = lax.rsqrt(sq / (4 * lw) + EPS)
        logits = jnp.zeros((tile, experts), f32)
        for b in range(4):
            normed = (hb[b, r, :].astype(f32) * inv * sm[b, experts : experts + 1, :].astype(f32)).astype(bf16)
            xn[r, b * lw : (b + 1) * lw] = normed
            logits = logits + lax.dot_general(
                normed, sm[b, 0:experts, :], (((1,), (1,)), ((), ())), preferred_element_type=f32
            )
        p = jnp.exp(logits - jnp.max(logits, axis=1, keepdims=True))
        p = p / jnp.sum(p, axis=1, keepdims=True)
        gates[r, :] = jnp.where(gates[r, :] > 0.0, p, 0.0)
        return 0

    lax.fori_loop(0, half // tile, route, 0)

    def piece(xs, fs, t):
        return acc.at[xs, rows(fs * 2 * quarter + t * part, part), :]

    def landing(slot, t):
        return rbuf.at[slot, rows(t * part, part), :]

    def along_x(src, slot, t):
        return remote(src, landing(slot, t), r_send.at[slot, t], r_recv.at[slot, t], f, 2 * (1 - x) + c)

    def along_y(src, slot, t):
        return remote(src, landing(slot, t), r_send.at[slot, t], r_recv.at[slot, t], 1 - f, i)

    lane_q = lax.broadcasted_iota(jnp.int32, (quarter, experts), 1)

    def expert(j, last):
        if not last:
            @pl.when(j + ahead < local_e)
            def _():
                send_expert(j + ahead)

        await_bytes(group(j), w_own.at[j])
        for d in (1, 2, 3):
            x2, f2, _q2 = chip(d)
            await_bytes(group(j), w_recv.at[j, d - 1])
            for ref in blocks(j, f2, 2 * x2 + c):
                remote(ref, ref, f_send.at[j, d], f_recv.at[j, d], f, sib).start()
        for d in range(4):
            await_bytes(group(j), f_recv.at[j, d])

        def step(n, _):
            r = rows((((1 - f) * 2 + n) % 4) * quarter, quarter)
            gate = jnp.sum(jnp.where(lane_q == local_e * q + j, gates[r, :], 0.0), axis=1, keepdims=True)
            for s in range(2):
                z0 = jnp.dot(xn[r, :], w0[j, s], preferred_element_type=f32).astype(bf16).astype(f32)
                z1 = jnp.dot(xn[r, :], w1[j, s], preferred_element_type=f32).astype(bf16).astype(f32)
                g = jnp.where(gate > 0.0, gelu_tanh(z0) * z1, 0.0)
                gb[:, s * fw : (s + 1) * fw] = g.astype(bf16)
            for b in range(4):
                y = jnp.dot(gb[...], w2[j, b], preferred_element_type=f32).astype(bf16).astype(f32)
                u = (y * gate).astype(bf16).astype(f32)
                acc[b // 2, r, (b % 2) * lw : (b % 2 + 1) * lw] += u

            if last:
                for k in range(4):
                    starts = [p for p in FIRST if p[2] == k]
                    if starts:
                        @pl.when(n == k)
                        def _():
                            for kind, t, _k in starts:
                                start_piece(kind, t)

            return 0

        lax.fori_loop(0, 4, step, 0)

    def start_piece(kind, t):
        along_first, along_last = (along_y, along_x) if t in Y_FIRST else (along_x, along_y)
        near = (x, 1 - f) if t in Y_FIRST else (1 - x, f)
        if kind == "D":
            along_first(piece(1 - x, 1 - f, t), 0, t).start()
        elif kind == "N":
            along_first(piece(*near, t), 1, t).start()
        else:
            far = (1 - x, f) if t in Y_FIRST else (x, 1 - f)
            along_last(piece(*far, t), 2, t).start()

    def experts_but_last(j, _):
        expert(j, False)
        return 0

    lax.fori_loop(0, local_e - 1, experts_but_last, 0)
    expert(local_e - 1, True)

    def add_to(xs, fs, t):
        r = rows(fs * 2 * quarter + t * part, part)
        await_bytes(landing(0, t), r_recv.at[0, t])
        acc[xs, r, :] = acc[xs, r, :] + rbuf[0, rows(t * part, part), :]

    def total(t):
        r = rows(f * 2 * quarter + t * part, part)
        s = rows(t * part, part)
        for slot in (1, 2):
            await_bytes(landing(slot, t), r_recv.at[slot, t])
        v = acc[x, r, :] + (rbuf[1, s, :] + rbuf[2, s, :])
        acc[x, r, :] = v
        v = v * v
        v = (v[:, 0:128] + v[:, 128:256]) + (v[:, 256:384] + v[:, 384:512])
        sq_own[t] = jnp.broadcast_to(jnp.sum(v.T, axis=0, keepdims=True), (8, part))
        remote(sq_own.at[t], sq_far.at[t], q_send.at[t], q_recv.at[t], f, 2 * (1 - x) + c).start()

    def out_rows(fs, cs, t):
        return out_ref.at[rows(cs * half + fs * 2 * quarter + t * part, part), :]

    def emit(t):
        r = rows(f * 2 * quarter + t * part, part)
        s = rows(t * part, part)
        await_bytes(sq_far.at[t], q_recv.at[t])
        inv = lax.rsqrt((sq_own[t, 0:1, :] + sq_far[t, 0:1, :]) / (4 * lw) + EPS)
        inv = jnp.broadcast_to(inv, (part, part)).T
        for b in range(2):
            post = sm[2 * x + b, experts + 1 : experts + 2, :].astype(f32)
            for g in range(lw // part):
                cols = slice(g * part, (g + 1) * part)
                m = acc[x, r, b * lw + g * part : b * lw + (g + 1) * part]
                hv = hb[2 * x + b, r, cols].astype(f32)
                ob[b, s, cols] = (hv + m * inv * post[:, cols]).astype(bf16)
        for b in range(2):
            remote(
                ob.at[b, s, :], out_rows(f, c, t), o_send.at[b, t], o_recv.at[c, t], 1 - f, 2 * x + b
            ).start()
        pltpu.make_async_copy(ob.at[c, s, :], out_rows(f, c, t), o_send.at[2, t]).start()
        remote(ob.at[1 - c, s, :], out_rows(f, c, t), o_send.at[3, t], o_recv.at[2, t], f, sib).start()

    for kind, t in REST:
        if kind == "m":
            add_to(*((1 - x, f) if t in Y_FIRST else (x, 1 - f)), t)
        elif kind == "t":
            total(t)
        elif kind == "e":
            emit(t)
        else:
            start_piece(kind, t)

    def close(t, _):
        here = ob.at[0, rows(t * part, part), :]
        for n in range(3):
            await_bytes(here, o_recv.at[n, t])
            await_bytes(landing(0, t), r_send.at[n, t])
        for n in range(4):
            await_bytes(here, o_send.at[n, t])
        await_bytes(sq_own.at[t], q_send.at[t])
        return 0

    lax.fori_loop(0, parts, close, 0)

    for n in range(3):
        await_bytes(sm.at[0], s_send.at[n])
    await_bytes(hb.at[0], h_send.at[2])
    for n in range(2):
        await_bytes(hb.at[0, across, :], h_send.at[n])
        await_bytes(hb.at[0, across, :], hf_send.at[n])

    def drain(j, _):
        for d in range(4):
            await_bytes(group(j), f_send.at[j, d])
            if d:
                await_bytes(group(j), w_send.at[j, d - 1])
        return 0

    lax.fori_loop(0, local_e, drain, 0)


def solution(mesh):
    emb_size = mesh.shape["emb"]
    ffn_size = mesh.shape["ffn"]
    assert emb_size == 4 and ffn_size == 2

    def local_block(hidden, norm_pre, norm_post, w_router, w_gate, w_up, w_down, choice):
        num_tok, lw = hidden.shape
        experts, _, fw = w_gate.shape
        top_k = choice.shape[1]
        capacity = 2 * num_tok * top_k // experts
        width, ffn = lw * emb_size, fw * ffn_size
        half, quarter, local_e = num_tok // 2, num_tok // 8, experts // 4
        small_rows = experts + 16
        row = lax.broadcasted_iota(jnp.int32, (small_rows, lw), 0)
        norms = jnp.where(row == experts, norm_pre[None, :], norm_post[None, :])
        small = jnp.where(row < experts, jnp.pad(w_router.T, ((0, 16), (0, 0))), norms)
        parts = 2 * quarter // 128
        bf16, f32 = jnp.bfloat16, jnp.float32
        dma = pltpu.SemaphoreType.DMA
        anywhere = pl.BlockSpec(memory_space=pl.ANY)
        flops = 2 * 3 * half * local_e * width * ffn
        return pl.pallas_call(
            functools.partial(kernel, experts, capacity),
            out_shape=jax.ShapeDtypeStruct((num_tok, lw), bf16),
            in_specs=[anywhere] * 5 + [pl.BlockSpec(memory_space=pltpu.VMEM)],
            out_specs=anywhere,
            scratch_shapes=[
                pltpu.VMEM((4, half, lw), bf16),
                pltpu.VMEM((4, small_rows, lw), bf16),
                pltpu.VMEM((local_e, 2, width, fw), bf16),
                pltpu.VMEM((local_e, 2, width, fw), bf16),
                pltpu.VMEM((local_e, 4, ffn, lw), bf16),
                pltpu.VMEM((half, width), bf16),
                pltpu.VMEM((half, experts), f32),
                pltpu.VMEM((2, half, width // 2), f32),
                pltpu.VMEM((3, 2 * quarter, width // 2), f32),
                pltpu.VMEM((parts, 8, 128), f32),
                pltpu.VMEM((parts, 8, 128), f32),
                pltpu.VMEM((2, 2 * quarter, lw), bf16),
                pltpu.VMEM((quarter, ffn), bf16),
                dma((3,)), dma((4,)), dma((2,)), dma((2,)), dma((3,)), dma((4,)),
                dma((local_e, 3)), dma((local_e, 3)), dma((local_e,)),
                dma((local_e, 4)), dma((local_e, 4)),
                dma((3, parts)), dma((3, parts)), dma((parts,)), dma((parts,)),
                dma((4, parts)), dma((3, parts)),
            ],
            compiler_params=pltpu.CompilerParams(
                collective_id=0, has_side_effects=True, vmem_limit_bytes=67043328
            ),
            cost_estimate=pl.CostEstimate(flops=flops, bytes_accessed=60 << 20, transcendentals=half * local_e * ffn),
        )(hidden, w_gate, w_up, w_down, small, choice.T)

    in_specs = (P('dp', 'emb'), P('emb'), P('emb'), P('emb', None), P(None, 'emb', 'ffn'), P(None, 'emb', 'ffn'), P(None, 'ffn', 'emb'), P('dp', None))
    return jax.shard_map(local_block, mesh=mesh, in_specs=in_specs, out_specs=P('dp', 'emb'), check_vma=False)
```

```python
import functools
import math

import jax
import jax.numpy as jnp
from jax import lax
from jax.experimental import pallas as pl
from jax.experimental.pallas import tpu as pltpu
from jax.sharding import PartitionSpec as P

EPS = 1e-5
LANES = 128
MESH = pl.DeviceIdType.MESH


PIECES = 16
Y_FIRST = (2, 6, 8, 10, 13)
ORDER = (
    "D3", "D0", "D1", "D2", "N2", "N6", "D5", "N13", "N5", "D6", "m2", "m3", "m0", "D7", "N10", "m1",
    "N0", "M3", "m5", "D4", "D10", "m6", "M6", "M1", "m7", "N1", "M0", "N11", "D13", "m4", "m10", "N3",
    "M4", "M2", "D8", "t0", "M7", "m13", "N4", "N8", "D12", "M5", "D9", "m8", "t1", "e0", "M8", "m12",
    "M12", "N9", "N7", "t2", "m9", "M9", "e1", "D11", "M10", "D15", "t4", "t3", "e2", "m11", "M11", "N12",
    "M13", "D14", "m15", "M15", "e3", "t5", "e4", "N14", "t6", "N15", "m14", "M14", "e5", "e6", "t7", "e7",
)


def plan():
    steps = [(p[0], int(p[1:])) for p in ORDER]
    head = next(n for n, p in enumerate(steps) if p[0] == "m")
    first, tile = [], 0
    for kind, t in steps[:head]:
        need = t // 4 + (4 if kind == "N" and t not in Y_FIRST else 0)
        tile = max(tile, need)
        first.append((kind, t, tile))
    return first, steps[head:]


FIRST, REST = plan()


def gelu_tanh(z):
    return z * (0.5 * (1.0 + jnp.tanh(math.sqrt(2.0 / math.pi) * (z + 0.044715 * (z * z * z)))))


def kernel(
    experts, capacity,
    h_ref, wg_ref, wu_ref, wd_ref, wr_ref, pre_ref, post_ref, choice_hbm, out_ref,
    choice_ref, hb, wr, pre, post, w0, w1, w2, xn, gates, acc, rbuf, sq_own, sq_far, ob, gb,
    h_send, h_recv, hf_send, hf_recv, s_send, s_recv, n_send, n_recv, c_sem, w_send, w_recv, w_own, f_send, f_recv,
    r_send, r_recv, q_send, q_recv, o_send, o_recv,
):
    num_tok, lw = h_ref.shape
    fw = wg_ref.shape[2]
    half = num_tok // 2
    quarter = num_tok // 8
    local_e = experts // 4
    tile = 256
    part = 128
    parts = quarter * 2 // part
    bf16, f32 = jnp.bfloat16, jnp.float32

    f = lax.axis_index("ffn")
    i = lax.axis_index("emb")
    x, c = i // 2, i % 2
    q = 2 * x + f
    sib = 2 * x + (1 - c)

    def chip(d):
        x2 = (x + d // 2) % 2
        f2 = (f + d % 2) % 2
        return x2, f2, 2 * x2 + f2

    def rows(start, size):
        return pl.ds(pl.multiple_of(start, 128), size)

    pltpu.make_async_copy(choice_hbm, choice_ref, c_sem).start()

    barrier = pltpu.get_barrier_semaphore()
    for df in range(2):
        for di in range(4):
            if df or di:
                pl.semaphore_signal(
                    barrier, inc=1, device_id={"ffn": (f + df) % 2, "emb": (i + di) % 4}, device_id_type=MESH
                )
    pl.semaphore_wait(barrier, 7)

    def remote(src, dst, send, recv, f2, i2):
        return pltpu.make_async_remote_copy(
            src_ref=src, dst_ref=dst, send_sem=send, recv_sem=recv,
            device_id={"ffn": f2, "emb": i2}, device_id_type=MESH,
        )

    def await_bytes(ref, sem):
        pltpu.make_async_copy(ref, ref, sem).wait()

    cols = pl.ds(pl.multiple_of(i * lw, 256), lw)

    def send_small(i2):
        remote(wr_ref, wr.at[i], s_send, s_recv.at[i], f, i2).start()
        remote(pre_ref, pre.at[cols], n_send.at[0], n_recv.at[0, i], f, i2).start()
        remote(post_ref, post.at[cols], n_send.at[1], n_recv.at[1, i], f, i2).start()

    own_h = pltpu.make_async_copy(h_ref.at[rows(c * half, half), :], hb.at[i], h_recv.at[i])
    own_h.start()
    pltpu.make_async_copy(wr_ref, wr.at[i], s_recv.at[i]).start()
    pltpu.make_async_copy(pre_ref, pre.at[cols], n_recv.at[0, i]).start()
    pltpu.make_async_copy(post_ref, post.at[cols], n_recv.at[1, i]).start()
    across = rows(f * (half // 2), half // 2)
    far = rows((1 - f) * (half // 2), half // 2)
    for c2 in range(2):
        i2 = 2 * (1 - x) + c2
        send_small(i2)
        src = h_ref.at[rows(c2 * half + f * (half // 2), half // 2), :]
        remote(src, hb.at[i, across, :], h_send.at[c2], h_recv.at[i], f, i2).start()
    send_small(sib)
    remote(h_ref.at[rows((1 - c) * half, half), :], hb.at[i], h_send.at[2], h_recv.at[i], f, sib).start()

    def blocks(j, fs, es):
        return (
            w0.at[j, fs, rows(es * lw, lw), :],
            w1.at[j, fs, rows(es * lw, lw), :],
            w2.at[j, es, rows(fs * fw, fw), :],
        )

    def group(j):
        return w0.at[j, 0, pl.ds(0, 3 * lw), :]

    def send_expert(j):
        dst = blocks(j, f, i)
        e = local_e * q + j
        for src, to in zip((wg_ref.at[e], wu_ref.at[e], wd_ref.at[e]), dst):
            pltpu.make_async_copy(src, to, w_own.at[j]).start()
            remote(src, to, f_send.at[0], f_recv.at[j, 0], f, sib).start()
        for m in range(3):
            for d in (3 - c, 2 + c, 1):
                x2, f2, q2 = chip(d)
                e2 = local_e * q2 + j
                src = (wg_ref.at[e2], wu_ref.at[e2], wd_ref.at[e2])[m]
                remote(src, dst[m], w_send.at[d - 1], w_recv.at[j, d - 1], f2, 2 * x2 + c).start()

    ahead = 3
    for j in range(2):
        send_expert(j)

    await_bytes(choice_ref, c_sem)

    sublane = lax.broadcasted_iota(jnp.int32, (experts, tile), 0)

    def chosen(start):
        ch = choice_ref[:, pl.ds(pl.multiple_of(start, LANES), tile)]
        a = jnp.zeros((experts, tile), f32)
        for k in range(choice_ref.shape[0]):
            a = a + jnp.where(ch[k : k + 1, :] == sublane, 1.0, 0.0)
        return a

    def count(n, total):
        return total + jnp.sum(chosen(n * tile), axis=1, keepdims=True)

    first = lax.fori_loop(0, half // tile, count, jnp.zeros((experts, 1), f32))
    strict = lax.broadcasted_iota(jnp.int32, (tile, tile), 0) < lax.broadcasted_iota(jnp.int32, (tile, tile), 1)
    strict = jnp.where(strict, 1.0, 0.0).astype(bf16)

    def place(n, carry):
        a = chosen(c * half + n * tile)
        before = carry + jnp.dot(a.astype(bf16), strict, preferred_element_type=f32)
        gates[rows(n * tile, tile), :] = jnp.where(before < capacity, a, 0.0).T
        for b in range(4):
            acc[b, rows(n * tile, tile), :] = jnp.zeros((tile, lw), f32)
        return carry + jnp.sum(a, axis=1, keepdims=True)

    lax.fori_loop(0, half // tile, place, first * c.astype(f32))

    for c2 in range(2):
        e2 = 2 * (1 - x) + c2
        await_bytes(hb.at[e2, across, :], h_recv.at[e2])
        ref = hb.at[e2, across, :]
        remote(ref, ref, hf_send.at[c2], hf_recv.at[c2], 1 - f, i).start()
    for j in range(2, ahead):
        send_expert(j)
    for c2 in range(2):
        await_bytes(hb.at[2 * x + c2], h_recv.at[2 * x + c2])
        await_bytes(hb.at[2 * (1 - x) + c2, far, :], hf_recv.at[c2])
    for b in range(4):
        await_bytes(wr.at[b], s_recv.at[b])
        for n, ref in enumerate((pre, post)):
            await_bytes(ref.at[pl.ds(b * lw, lw)], n_recv.at[n, b])

    def route(n, _):
        r = rows(n * tile, tile)
        sq = jnp.zeros((tile, 1), f32)
        for b in range(4):
            hv = hb[b, r, :].astype(f32)
            sq = sq + jnp.sum(hv * hv, axis=1, keepdims=True)
        inv = lax.rsqrt(sq / (4 * lw) + EPS)
        logits = jnp.zeros((tile, experts), f32)
        for b in range(4):
            normed = (hb[b, r, :].astype(f32) * inv * pre[b * lw : (b + 1) * lw].astype(f32)[None, :]).astype(bf16)
            xn[r, b * lw : (b + 1) * lw] = normed
            logits = logits + lax.dot_general(
                normed, wr[b], (((1,), (1,)), ((), ())), preferred_element_type=f32
            )
        p = jnp.exp(logits - jnp.max(logits, axis=1, keepdims=True))
        p = p / jnp.sum(p, axis=1, keepdims=True)
        gates[r, :] = jnp.where(gates[r, :] > 0.0, p, 0.0)
        return 0

    lax.fori_loop(0, half // tile, route, 0)

    def piece(xs, fs, t):
        return acc.at[2 * xs + t % 2, rows(fs * 2 * quarter + t // 2 * part, part), :]

    def landing(slot, t):
        return rbuf.at[slot, t % 2, rows(t // 2 * part, part), :]

    def along_x(src, slot, t):
        return remote(src, landing(slot, t), r_send.at[slot], r_recv.at[slot, t], f, 2 * (1 - x) + c)

    def along_y(src, slot, t):
        return remote(src, landing(slot, t), r_send.at[slot], r_recv.at[slot, t], 1 - f, i)

    lane_q = lax.broadcasted_iota(jnp.int32, (quarter, experts), 1)

    def expert(j, last):
        if not last:
            @pl.when(j + ahead < local_e)
            def _():
                send_expert(j + ahead)

        await_bytes(group(j), w_own.at[j])
        for d in (1, 2, 3):
            x2, f2, _q2 = chip(d)
            await_bytes(group(j), w_recv.at[j, d - 1])
            for ref in blocks(j, f2, 2 * x2 + c):
                remote(ref, ref, f_send.at[d], f_recv.at[j, d], f, sib).start()
        for d in range(4):
            await_bytes(group(j), f_recv.at[j, d])

        count = 8 if last else 4
        size = half // count

        def step(n, _):
            r = rows((((1 - f) * count // 2 + n) % count) * size, size)
            gate = jnp.sum(jnp.where(lane_q[0:size] == local_e * q + j, gates[r, :], 0.0), axis=1, keepdims=True)
            for s in range(2):
                z0 = jnp.dot(xn[r, :], w0[j, s], preferred_element_type=f32).astype(bf16).astype(f32)
                z1 = jnp.dot(xn[r, :], w1[j, s], preferred_element_type=f32).astype(bf16).astype(f32)
                g = jnp.where(gate > 0.0, gelu_tanh(z0) * z1, 0.0)
                gb[0:size, s * fw : (s + 1) * fw] = g.astype(bf16)
            for b in range(4):
                y = jnp.dot(gb[0:size, :], w2[j, b], preferred_element_type=f32).astype(bf16).astype(f32)
                u = (y * gate).astype(bf16).astype(f32)
                acc[b, r, :] += u

            if last:
                for k in range(count):
                    starts = [p for p in FIRST if p[2] == k]
                    if starts:
                        @pl.when(n == k)
                        def _():
                            for kind, t, _k in starts:
                                start_piece(kind, t)

            return 0

        lax.fori_loop(0, count, step, 0)

    def start_piece(kind, t):
        along_first, along_last = (along_y, along_x) if t in Y_FIRST else (along_x, along_y)
        near = (x, 1 - f) if t in Y_FIRST else (1 - x, f)
        if kind == "D":
            along_first(piece(1 - x, 1 - f, t), 0, t).start()
        elif kind == "N":
            along_first(piece(*near, t), 1, t).start()
        else:
            far = (1 - x, f) if t in Y_FIRST else (x, 1 - f)
            along_last(piece(*far, t), 2, t).start()

    def experts_but_last(j, _):
        expert(j, False)
        return 0

    lax.fori_loop(0, local_e - 1, experts_but_last, 0)
    expert(local_e - 1, True)

    def add_to(xs, fs, t):
        here = piece(xs, fs, t)
        await_bytes(landing(0, t), r_recv.at[0, t])
        here[...] = here[...] + landing(0, t)[...]

    def total(t):
        r = rows(f * 2 * quarter + t * part, part)
        s = rows(t * part, part)
        sq = jnp.zeros((part, part), f32)
        for b in range(2):
            for slot in (1, 2):
                await_bytes(landing(slot, 2 * t + b), r_recv.at[slot, 2 * t + b])
            v = acc[2 * x + b, r, :] + (rbuf[1, b, s, :] + rbuf[2, b, s, :])
            acc[2 * x + b, r, :] = v
            v = v * v
            sq = sq + (v[:, 0:128] + v[:, 128:256])
        sq_own[t] = jnp.broadcast_to(jnp.sum(sq.T, axis=0, keepdims=True), (8, part))
        remote(sq_own.at[t], sq_far.at[t], q_send, q_recv.at[t], f, 2 * (1 - x) + c).start()

    def out_rows(fs, cs, t):
        return out_ref.at[rows(cs * half + fs * 2 * quarter + t * part, part), :]

    def emit(t):
        r = rows(f * 2 * quarter + t * part, part)
        s = rows(t * part, part)
        await_bytes(sq_far.at[t], q_recv.at[t])
        inv = lax.rsqrt((sq_own[t, 0:1, :] + sq_far[t, 0:1, :]) / (4 * lw) + EPS)
        inv = jnp.broadcast_to(inv, (part, part)).T
        for b in range(2):
            gain = post[pl.ds(pl.multiple_of((2 * x + b) * lw, 256), lw)].astype(f32)[None, :]
            for g in range(lw // part):
                cols = slice(g * part, (g + 1) * part)
                m = acc[2 * x + b, r, cols]
                hv = hb[2 * x + b, r, cols].astype(f32)
                ob[b, s, cols] = (hv + m * inv * gain[:, cols]).astype(bf16)
        for b in range(2):
            remote(
                ob.at[b, s, :], out_rows(f, c, t), o_send.at[b], o_recv.at[c, t], 1 - f, 2 * x + b
            ).start()
        own = rows(c * half + f * 2 * quarter + t * part, part)
        out_ref[own, :] = ob[c, s, :]
        remote(ob.at[1 - c, s, :], out_rows(f, c, t), o_send.at[2], o_recv.at[2, t], f, sib).start()

    for kind, t in REST:
        if kind == "m":
            add_to(*((1 - x, f) if t in Y_FIRST else (x, 1 - f)), t)
        elif kind == "t":
            total(t)
        elif kind == "e":
            emit(t)
        else:
            start_piece(kind, t)

    def close(t, _):
        here = ob.at[0, rows(t * part, part), :]
        for n in range(3):
            await_bytes(here, o_recv.at[n, t])
        return 0

    lax.fori_loop(0, parts, close, 0)
    for n in range(3):
        await_bytes(ob.at[0], o_send.at[n])
        await_bytes(rbuf.at[0], r_send.at[n])
    await_bytes(sq_own, q_send)

    await_bytes(wr.at[pl.ds(0, 3)], s_send)
    for n in range(2):
        await_bytes(pre.at[pl.ds(0, 3 * lw)], n_send.at[n])
    await_bytes(hb.at[0], h_send.at[2])
    for n in range(2):
        await_bytes(hb.at[0, across, :], h_send.at[n])
        await_bytes(hb.at[0, across, :], hf_send.at[n])

    sent = w0.at[pl.ds(0, 3 * local_e // 8)]
    for d in range(4):
        await_bytes(sent, f_send.at[d])
        if d:
            await_bytes(sent, w_send.at[d - 1])


def solution(mesh):
    emb_size = mesh.shape["emb"]
    ffn_size = mesh.shape["ffn"]
    assert emb_size == 4 and ffn_size == 2

    def local_block(hidden, norm_pre, norm_post, w_router, w_gate, w_up, w_down, choice):
        num_tok, lw = hidden.shape
        experts, _, fw = w_gate.shape
        top_k = choice.shape[1]
        capacity = 2 * num_tok * top_k // experts
        width, ffn = lw * emb_size, fw * ffn_size
        half, quarter, local_e = num_tok // 2, num_tok // 8, experts // 4
        parts = 2 * quarter // 128
        bf16, f32 = jnp.bfloat16, jnp.float32
        dma = pltpu.SemaphoreType.DMA
        anywhere = pl.BlockSpec(memory_space=pl.ANY)
        flops = 2 * 3 * half * local_e * width * ffn
        return pl.pallas_call(
            functools.partial(kernel, experts, capacity),
            out_shape=pltpu.VMEM((num_tok, lw), bf16),
            in_specs=[anywhere] * 8,
            out_specs=pl.BlockSpec(memory_space=pltpu.VMEM),
            scratch_shapes=[
                pltpu.VMEM((top_k, num_tok), jnp.int32),
                pltpu.VMEM((4, half, lw), bf16),
                pltpu.VMEM((4, experts, lw), bf16),
                pltpu.VMEM((width,), bf16),
                pltpu.VMEM((width,), bf16),
                pltpu.VMEM((local_e, 2, width, fw), bf16),
                pltpu.VMEM((local_e, 2, width, fw), bf16),
                pltpu.VMEM((local_e, 4, ffn, lw), bf16),
                pltpu.VMEM((half, width), bf16),
                pltpu.VMEM((half, experts), f32),
                pltpu.VMEM((4, half, lw), f32),
                pltpu.VMEM((3, 2, 2 * quarter, lw), f32),
                pltpu.VMEM((parts, 8, 128), f32),
                pltpu.VMEM((parts, 8, 128), f32),
                pltpu.VMEM((2, 2 * quarter, lw), bf16),
                pltpu.VMEM((quarter, ffn), bf16),
                dma((3,)), dma((4,)), dma((2,)), dma((2,)), dma(()), dma((4,)), dma((2,)), dma((2, 4)), dma(()),
                dma((3,)), dma((local_e, 3)), dma((local_e,)),
                dma((4,)), dma((local_e, 4)),
                dma((3,)), dma((3, 2 * parts)), dma(()), dma((parts,)),
                dma((3,)), dma((3, parts)),
            ],
            compiler_params=pltpu.CompilerParams(
                collective_id=0, has_side_effects=True, vmem_limit_bytes=58 << 20
            ),
            cost_estimate=pl.CostEstimate(flops=flops, bytes_accessed=60 << 20, transcendentals=half * local_e * ffn),
        )(hidden, w_gate, w_up, w_down, w_router.T, norm_pre, norm_post, choice.T)

    in_specs = (P('dp', 'emb'), P('emb'), P('emb'), P('emb', None), P(None, 'emb', 'ffn'), P(None, 'emb', 'ffn'), P(None, 'ffn', 'emb'), P('dp', None))
    return jax.shard_map(local_block, mesh=mesh, in_specs=in_specs, out_specs=P('dp', 'emb'), check_vma=False)
```

```python
import functools
import math

import jax
import jax.numpy as jnp
from jax import lax
from jax.experimental import pallas as pl
from jax.experimental.pallas import tpu as pltpu
from jax.sharding import PartitionSpec as P

EPS = 1e-5
LANES = 128
MESH = pl.DeviceIdType.MESH


PIECES = 16
Y_FIRST = (2, 6, 8, 10, 13)
ORDER = (
    "D3", "D0", "D1", "D2", "N2", "N6", "D5", "N13", "N5", "D6", "m2", "m3", "m0", "D7", "N10", "m1",
    "N0", "M3", "m5", "D4", "D10", "m6", "M6", "M1", "m7", "N1", "M0", "N11", "D13", "m4", "m10", "N3",
    "M4", "M2", "D8", "t0", "M7", "m13", "N4", "N8", "D12", "M5", "D9", "m8", "t1", "e0", "M8", "m12",
    "M12", "N9", "N7", "t2", "m9", "M9", "e1", "D11", "M10", "D15", "t4", "t3", "e2", "m11", "M11", "N12",
    "M13", "D14", "m15", "M15", "e3", "t5", "e4", "N14", "t6", "N15", "m14", "M14", "e5", "e6", "t7", "e7",
)


def plan():
    steps = [(p[0], int(p[1:])) for p in ORDER]
    head = next(n for n, p in enumerate(steps) if p[0] == "m")
    first, tile = [], 0
    for kind, t in steps[:head]:
        need = t // 4 + (4 if kind == "N" and t not in Y_FIRST else 0)
        tile = max(tile, need)
        first.append((kind, t, tile))
    return first, steps[head:]


FIRST, REST = plan()


def gelu_tanh(z):
    return z * (0.5 * (1.0 + jnp.tanh(math.sqrt(2.0 / math.pi) * (z + 0.044715 * (z * z * z)))))


def kernel(
    experts, capacity,
    h_ref, wg_ref, wu_ref, wd_ref, wr_ref, pre_ref, post_ref, choice_hbm, out_ref,
    choice_ref, hb, wr, pre, post, w0, w1, w2, xn, gates, acc, rbuf, sq_own, sq_far, ob, gb,
    h_send, h_recv, hf_send, hf_recv, s_send, s_recv, n_send, n_recv, c_sem, w_send, w_recv, w_own, f_own, f_send, f_recv,
    r_send, r_recv, q_send, q_recv, o_send, o_recv,
):
    num_tok, lw = h_ref.shape
    fw = wg_ref.shape[2]
    half = num_tok // 2
    quarter = num_tok // 8
    local_e = experts // 4
    tile = 256
    part = 128
    parts = quarter * 2 // part
    bf16, f32 = jnp.bfloat16, jnp.float32

    f = lax.axis_index("ffn")
    i = lax.axis_index("emb")
    x, c = i // 2, i % 2
    q = 2 * x + f
    sib = 2 * x + (1 - c)

    def chip(d):
        x2 = (x + d // 2) % 2
        f2 = (f + d % 2) % 2
        return x2, f2, 2 * x2 + f2

    def rows(start, size):
        return pl.ds(pl.multiple_of(start, 128), size)

    pltpu.make_async_copy(choice_hbm, choice_ref, c_sem).start()

    barrier = pltpu.get_barrier_semaphore()
    for f2, i2 in (
        (1 - f, 2 * (1 - x) + c), (1 - f, 2 * (1 - x) + 1 - c), (1 - f, i), (1 - f, sib),
        (f, 2 * (1 - x) + c), (f, 2 * (1 - x) + 1 - c), (f, sib),
    ):
        pl.semaphore_signal(barrier, inc=1, device_id={"ffn": f2, "emb": i2}, device_id_type=MESH)
    pl.semaphore_wait(barrier, 7)

    def remote(src, dst, send, recv, f2, i2):
        return pltpu.make_async_remote_copy(
            src_ref=src, dst_ref=dst, send_sem=send, recv_sem=recv,
            device_id={"ffn": f2, "emb": i2}, device_id_type=MESH,
        )

    def await_bytes(ref, sem):
        pltpu.make_async_copy(ref, ref, sem).wait()

    cols = pl.ds(pl.multiple_of(i * lw, 256), lw)

    def send_small(i2):
        remote(wr_ref, wr.at[i], s_send, s_recv.at[i], f, i2).start()
        remote(pre_ref, pre.at[cols], n_send.at[0], n_recv.at[0, i], f, i2).start()
        remote(post_ref, post.at[cols], n_send.at[1], n_recv.at[1, i], f, i2).start()

    own_h = pltpu.make_async_copy(h_ref.at[rows(c * half, half), :], hb.at[i], h_recv.at[i])
    own_h.start()
    pltpu.make_async_copy(wr_ref, wr.at[i], s_recv.at[i]).start()
    pltpu.make_async_copy(pre_ref, pre.at[cols], n_recv.at[0, i]).start()
    pltpu.make_async_copy(post_ref, post.at[cols], n_recv.at[1, i]).start()
    across = rows(f * (half // 2), half // 2)
    far = rows((1 - f) * (half // 2), half // 2)
    for c2 in range(2):
        i2 = 2 * (1 - x) + c2
        send_small(i2)
        src = h_ref.at[rows(c2 * half + f * (half // 2), half // 2), :]
        remote(src, hb.at[i, across, :], h_send.at[c2], h_recv.at[i], f, i2).start()
    send_small(sib)
    remote(h_ref.at[rows((1 - c) * half, half), :], hb.at[i], h_send.at[2], h_recv.at[i], f, sib).start()

    def blocks(j, fs, es):
        return (
            w0.at[j, fs, rows(es * lw, lw), :],
            w1.at[j, fs, rows(es * lw, lw), :],
            w2.at[j, es, rows(fs * fw, fw), :],
        )

    def group(j):
        return w0.at[j, 0, pl.ds(0, 3 * lw), :]

    mine = pl.ds(local_e * q, local_e)
    own_blocks = (
        w0.at[:, f, rows(i * lw, lw), :],
        w1.at[:, f, rows(i * lw, lw), :],
        w2.at[:, i, rows(f * fw, fw), :],
    )
    for src, to in zip((wg_ref.at[mine], wu_ref.at[mine], wd_ref.at[mine]), own_blocks):
        pltpu.make_async_copy(src, to, w_own).start()
        remote(src, to, f_send.at[0], f_own, f, sib).start()

    def send_block(j, m, d):
        x2, f2, q2 = chip(d)
        src = (wg_ref, wu_ref, wd_ref)[m].at[local_e * q2 + j]
        remote(src, blocks(j, f, i)[m], w_send.at[d - 1], w_recv.at[j, d - 1], f2, 2 * x2 + c).start()

    def send_expert(j, skip=0):
        for m in range(3):
            for d in (3 - c, 2 + c) + (() if m < skip else (1,)):
                send_block(j, m, d)

    ahead, begun = 3, 2
    for j in range(2):
        send_expert(j)
    for m in range(begun):
        send_block(2, m, 1)

    await_bytes(choice_ref, c_sem)

    sublane = lax.broadcasted_iota(jnp.int32, (experts, tile), 0)

    def chosen(start):
        ch = choice_ref[:, pl.ds(pl.multiple_of(start, LANES), tile)]
        a = jnp.zeros((experts, tile), f32)
        for k in range(choice_ref.shape[0]):
            a = a + jnp.where(ch[k : k + 1, :] == sublane, 1.0, 0.0)
        return a

    def count(n, total):
        return total + jnp.sum(chosen(n * tile), axis=1, keepdims=True)

    first = lax.fori_loop(0, half // tile, count, jnp.zeros((experts, 1), f32))
    strict = lax.broadcasted_iota(jnp.int32, (tile, tile), 0) < lax.broadcasted_iota(jnp.int32, (tile, tile), 1)
    strict = jnp.where(strict, 1.0, 0.0).astype(bf16)

    def place(n, carry):
        a = chosen(c * half + n * tile)
        before = carry + jnp.dot(a.astype(bf16), strict, preferred_element_type=f32)
        gates[rows(n * tile, tile), :] = jnp.where(before < capacity, a, 0.0).T
        for b in range(4):
            acc[b, rows(n * tile, tile), :] = jnp.zeros((tile, lw), f32)
        return carry + jnp.sum(a, axis=1, keepdims=True)

    lax.fori_loop(0, half // tile, place, first * c.astype(f32))

    for c2 in range(2):
        e2 = 2 * (1 - x) + c2
        await_bytes(hb.at[e2, across, :], h_recv.at[e2])
        ref = hb.at[e2, across, :]
        remote(ref, ref, hf_send.at[c2], hf_recv.at[c2], 1 - f, i).start()
    for j in range(2, ahead):
        send_expert(j, begun if j == 2 else 0)
    for c2 in range(2):
        await_bytes(hb.at[2 * x + c2], h_recv.at[2 * x + c2])
        await_bytes(hb.at[2 * (1 - x) + c2, far, :], hf_recv.at[c2])
    for b in range(4):
        await_bytes(wr.at[b], s_recv.at[b])
        for n, ref in enumerate((pre, post)):
            await_bytes(ref.at[pl.ds(b * lw, lw)], n_recv.at[n, b])

    def forward(j):
        for d in (1, 3, 2):
            x2, f2, _q2 = chip(d)
            await_bytes(group(j), w_recv.at[j, d - 1])
            for ref in blocks(j, f2, 2 * x2 + c):
                remote(ref, ref, f_send.at[d], f_recv.at[j, d - 1], f, sib).start()

    forward(0)

    def route(n, _):
        r = rows(n * tile, tile)
        sq = jnp.zeros((tile, 1), f32)
        for b in range(4):
            hv = hb[b, r, :].astype(f32)
            sq = sq + jnp.sum(hv * hv, axis=1, keepdims=True)
        inv = lax.rsqrt(sq / (4 * lw) + EPS)
        logits = jnp.zeros((tile, experts), f32)
        for b in range(4):
            normed = (hb[b, r, :].astype(f32) * inv * pre[b * lw : (b + 1) * lw].astype(f32)[None, :]).astype(bf16)
            xn[r, b * lw : (b + 1) * lw] = normed
            logits = logits + lax.dot_general(
                normed, wr[b], (((1,), (1,)), ((), ())), preferred_element_type=f32
            )
        p = jnp.exp(logits - jnp.max(logits, axis=1, keepdims=True))
        p = p / jnp.sum(p, axis=1, keepdims=True)
        gates[r, :] = jnp.where(gates[r, :] > 0.0, p, 0.0)
        return 0

    lax.fori_loop(0, half // tile, route, 0)

    def piece(xs, fs, t):
        return acc.at[2 * xs + t % 2, rows(fs * 2 * quarter + t // 2 * part, part), :]

    def landing(slot, t):
        return rbuf.at[slot, t % 2, rows(t // 2 * part, part), :]

    def along_x(src, slot, t):
        return remote(src, landing(slot, t), r_send.at[slot], r_recv.at[slot, t], f, 2 * (1 - x) + c)

    def along_y(src, slot, t):
        return remote(src, landing(slot, t), r_send.at[slot], r_recv.at[slot, t], 1 - f, i)

    sent = w0.at[pl.ds(0, 3 * local_e // 8)]
    await_bytes(sent, w_own)
    await_bytes(sent, f_own)

    lane_q = lax.broadcasted_iota(jnp.int32, (quarter, experts), 1)

    def expert(j, last):
        if not last:
            @pl.when(j + ahead < local_e)
            def _():
                send_expert(j + ahead)

        if last:
            forward(j)
        else:
            @pl.when(j >= 1)
            def _():
                forward(j)

        for d in (1, 2, 3):
            await_bytes(group(j), f_recv.at[j, d - 1])

        count = 8 if last else 4
        size = half // count

        def step(n, _):
            r = rows((((1 - f) * count // 2 + n) % count) * size, size)
            gate = jnp.sum(jnp.where(lane_q[0:size] == local_e * q + j, gates[r, :], 0.0), axis=1, keepdims=True)
            for s in range(2):
                z0 = jnp.dot(xn[r, :], w0[j, s], preferred_element_type=f32).astype(bf16).astype(f32)
                z1 = jnp.dot(xn[r, :], w1[j, s], preferred_element_type=f32).astype(bf16).astype(f32)
                g = jnp.where(gate > 0.0, gelu_tanh(z0) * z1, 0.0)
                gb[0:size, s * fw : (s + 1) * fw] = g.astype(bf16)
            for b in range(4):
                y = jnp.dot(gb[0:size, :], w2[j, b], preferred_element_type=f32).astype(bf16).astype(f32)
                u = (y * gate).astype(bf16).astype(f32)
                acc[b, r, :] += u

            if last:
                for k in range(count):
                    starts = [p for p in FIRST if p[2] == k]
                    if starts:
                        @pl.when(n == k)
                        def _():
                            for kind, t, _k in starts:
                                start_piece(kind, t)

            return 0

        lax.fori_loop(0, count, step, 0)

    def start_piece(kind, t):
        along_first, along_last = (along_y, along_x) if t in Y_FIRST else (along_x, along_y)
        near = (x, 1 - f) if t in Y_FIRST else (1 - x, f)
        if kind == "D":
            along_first(piece(1 - x, 1 - f, t), 0, t).start()
        elif kind == "N":
            along_first(piece(*near, t), 1, t).start()
        else:
            far = (1 - x, f) if t in Y_FIRST else (x, 1 - f)
            along_last(piece(*far, t), 2, t).start()

    def experts_but_last(j, _):
        expert(j, False)
        return 0

    lax.fori_loop(0, local_e - 1, experts_but_last, 0)
    expert(local_e - 1, True)

    def add_to(xs, fs, t):
        here = piece(xs, fs, t)
        await_bytes(landing(0, t), r_recv.at[0, t])
        here[...] = here[...] + landing(0, t)[...]

    def total(t):
        r = rows(f * 2 * quarter + t * part, part)
        s = rows(t * part, part)
        sq = jnp.zeros((part, part), f32)
        for b in range(2):
            for slot in (1, 2):
                await_bytes(landing(slot, 2 * t + b), r_recv.at[slot, 2 * t + b])
            v = acc[2 * x + b, r, :] + (rbuf[1, b, s, :] + rbuf[2, b, s, :])
            acc[2 * x + b, r, :] = v
            v = v * v
            sq = sq + (v[:, 0:128] + v[:, 128:256])
        sq_own[t] = jnp.broadcast_to(jnp.sum(sq.T, axis=0, keepdims=True), (8, part))
        remote(sq_own.at[t], sq_far.at[t], q_send, q_recv.at[t], f, 2 * (1 - x) + c).start()

    def out_rows(fs, cs, t):
        return out_ref.at[rows(cs * half + fs * 2 * quarter + t * part, part), :]

    def emit(t):
        r = rows(f * 2 * quarter + t * part, part)
        s = rows(t * part, part)
        await_bytes(sq_far.at[t], q_recv.at[t])
        inv = lax.rsqrt((sq_own[t, 0:1, :] + sq_far[t, 0:1, :]) / (4 * lw) + EPS)
        inv = jnp.broadcast_to(inv, (part, part)).T
        for b in range(2):
            gain = post[pl.ds(pl.multiple_of((2 * x + b) * lw, 256), lw)].astype(f32)[None, :]
            for g in range(lw // part):
                cols = slice(g * part, (g + 1) * part)
                m = acc[2 * x + b, r, cols]
                hv = hb[2 * x + b, r, cols].astype(f32)
                ob[b, s, cols] = (hv + m * inv * gain[:, cols]).astype(bf16)
        for b in range(2):
            remote(
                ob.at[b, s, :], out_rows(f, c, t), o_send.at[b], o_recv.at[c, t], 1 - f, 2 * x + b
            ).start()
        own = rows(c * half + f * 2 * quarter + t * part, part)
        out_ref[own, :] = ob[c, s, :]
        remote(ob.at[1 - c, s, :], out_rows(f, c, t), o_send.at[2], o_recv.at[2, t], f, sib).start()

    for kind, t in REST:
        if kind == "m":
            add_to(*((1 - x, f) if t in Y_FIRST else (x, 1 - f)), t)
        elif kind == "t":
            total(t)
        elif kind == "e":
            emit(t)
        else:
            start_piece(kind, t)

    def close(t, _):
        here = ob.at[0, rows(t * part, part), :]
        for n in range(3):
            await_bytes(here, o_recv.at[n, t])
        return 0

    lax.fori_loop(0, parts, close, 0)
    for n in range(3):
        await_bytes(ob.at[0], o_send.at[n])
        await_bytes(rbuf.at[0], r_send.at[n])
    await_bytes(sq_own, q_send)

    await_bytes(wr.at[pl.ds(0, 3)], s_send)
    for n in range(2):
        await_bytes(pre.at[pl.ds(0, 3 * lw)], n_send.at[n])
    await_bytes(hb.at[0], h_send.at[2])
    for n in range(2):
        await_bytes(hb.at[0, across, :], h_send.at[n])
        await_bytes(hb.at[0, across, :], hf_send.at[n])

    for d in range(4):
        await_bytes(sent, f_send.at[d])
        if d:
            await_bytes(sent, w_send.at[d - 1])


def solution(mesh):
    emb_size = mesh.shape["emb"]
    ffn_size = mesh.shape["ffn"]
    assert emb_size == 4 and ffn_size == 2

    def local_block(hidden, norm_pre, norm_post, w_router, w_gate, w_up, w_down, choice):
        num_tok, lw = hidden.shape
        experts, _, fw = w_gate.shape
        top_k = choice.shape[1]
        capacity = 2 * num_tok * top_k // experts
        width, ffn = lw * emb_size, fw * ffn_size
        half, quarter, local_e = num_tok // 2, num_tok // 8, experts // 4
        parts = 2 * quarter // 128
        bf16, f32 = jnp.bfloat16, jnp.float32
        dma = pltpu.SemaphoreType.DMA
        anywhere = pl.BlockSpec(memory_space=pl.ANY)
        flops = 2 * 3 * half * local_e * width * ffn
        return pl.pallas_call(
            functools.partial(kernel, experts, capacity),
            out_shape=pltpu.VMEM((num_tok, lw), bf16),
            in_specs=[anywhere] * 8,
            out_specs=pl.BlockSpec(memory_space=pltpu.VMEM),
            scratch_shapes=[
                pltpu.VMEM((top_k, num_tok), jnp.int32),
                pltpu.VMEM((4, half, lw), bf16),
                pltpu.VMEM((4, experts, lw), bf16),
                pltpu.VMEM((width,), bf16),
                pltpu.VMEM((width,), bf16),
                pltpu.VMEM((local_e, 2, width, fw), bf16),
                pltpu.VMEM((local_e, 2, width, fw), bf16),
                pltpu.VMEM((local_e, 4, ffn, lw), bf16),
                pltpu.VMEM((half, width), bf16),
                pltpu.VMEM((half, experts), f32),
                pltpu.VMEM((4, half, lw), f32),
                pltpu.VMEM((3, 2, 2 * quarter, lw), f32),
                pltpu.VMEM((parts, 8, 128), f32),
                pltpu.VMEM((parts, 8, 128), f32),
                pltpu.VMEM((2, 2 * quarter, lw), bf16),
                pltpu.VMEM((quarter, ffn), bf16),
                dma((3,)), dma((4,)), dma((2,)), dma((2,)), dma(()), dma((4,)), dma((2,)), dma((2, 4)), dma(()),
                dma((3,)), dma((local_e, 3)), dma(()), dma(()),
                dma((4,)), dma((local_e, 3)),
                dma((3,)), dma((3, 2 * parts)), dma(()), dma((parts,)),
                dma((3,)), dma((3, parts)),
            ],
            compiler_params=pltpu.CompilerParams(
                collective_id=0, has_side_effects=True, vmem_limit_bytes=58 << 20
            ),
            cost_estimate=pl.CostEstimate(flops=flops, bytes_accessed=60 << 20, transcendentals=half * local_e * ffn),
        )(hidden, w_gate, w_up, w_down, w_router.T, norm_pre, norm_post, choice.T)

    in_specs = (P('dp', 'emb'), P('emb'), P('emb'), P('emb', None), P(None, 'emb', 'ffn'), P(None, 'emb', 'ffn'), P(None, 'ffn', 'emb'), P('dp', None))
    return jax.shard_map(local_block, mesh=mesh, in_specs=in_specs, out_specs=P('dp', 'emb'), check_vma=False)
```

```python
import functools
import math

import jax
import jax.numpy as jnp
from jax import lax
from jax.experimental import pallas as pl
from jax.experimental.pallas import tpu as pltpu
from jax.sharding import PartitionSpec as P

EPS = 1e-5
LANES = 128
MESH = pl.DeviceIdType.MESH


PIECES = 16
Y_FIRST = (2, 6, 8, 10, 13)
ORDER = (
    "D3", "D0", "D1", "D2", "N2", "N6", "D5", "N13", "N5", "D6", "m2", "m3", "m0", "D7", "N10", "m1",
    "N0", "M3", "m5", "D4", "D10", "m6", "M6", "M1", "m7", "N1", "M0", "N11", "D13", "m4", "m10", "N3",
    "M4", "M2", "D8", "t0", "M7", "m13", "N4", "N8", "D12", "M5", "D9", "m8", "t1", "e0", "M8", "m12",
    "M12", "N9", "N7", "t2", "m9", "M9", "e1", "D11", "M10", "D15", "t4", "t3", "e2", "m11", "M11", "N12",
    "M13", "D14", "m15", "M15", "e3", "t5", "e4", "N14", "t6", "N15", "m14", "M14", "e5", "e6", "t7", "e7",
)


def plan():
    steps = [(p[0], int(p[1:])) for p in ORDER]
    head = next(n for n, p in enumerate(steps) if p[0] == "m")
    first, tile = [], 0
    for kind, t in steps[:head]:
        need = t // 4 + (4 if kind == "N" and t not in Y_FIRST else 0)
        tile = max(tile, need)
        first.append((kind, t, tile))
    return first, steps[head:]


FIRST, REST = plan()


def gelu_tanh(z):
    return z * (0.5 * (1.0 + jnp.tanh(math.sqrt(2.0 / math.pi) * (z + 0.044715 * (z * z * z)))))


def kernel(
    experts, capacity,
    h_ref, wg_ref, wu_ref, wd_ref, wr_ref, pre_ref, post_ref, choice_hbm, out_ref,
    choice_ref, hb, wr, pre, post, w0, w1, w2, xn, gates, acc, rbuf, sq_own, sq_far, ob, gb,
    h_send, h_recv, hf_send, hf_recv, s_send, s_recv, n_send, n_recv, c_sem, w_send, w_recv, w_own, f_own, f_send, f_recv,
    r_send, r_recv, q_send, q_recv, o_send, o_recv,
):
    num_tok, lw = h_ref.shape
    fw = wg_ref.shape[2]
    half = num_tok // 2
    quarter = num_tok // 8
    local_e = experts // 4
    tile = 256
    part = 128
    parts = quarter * 2 // part
    bf16, f32 = jnp.bfloat16, jnp.float32

    f = lax.axis_index("ffn")
    i = lax.axis_index("emb")
    x, c = i // 2, i % 2
    q = 2 * x + f
    sib = 2 * x + (1 - c)

    def chip(d):
        x2 = (x + d // 2) % 2
        f2 = (f + d % 2) % 2
        return x2, f2, 2 * x2 + f2

    def rows(start, size):
        return pl.ds(pl.multiple_of(start, 128), size)

    pltpu.make_async_copy(choice_hbm, choice_ref, c_sem).start()

    barrier = pltpu.get_barrier_semaphore()
    for f2, i2 in (
        (1 - f, 2 * (1 - x) + c), (1 - f, 2 * (1 - x) + 1 - c), (1 - f, i), (1 - f, sib),
        (f, 2 * (1 - x) + c), (f, 2 * (1 - x) + 1 - c), (f, sib),
    ):
        pl.semaphore_signal(barrier, inc=1, device_id={"ffn": f2, "emb": i2}, device_id_type=MESH)
    pl.semaphore_wait(barrier, 7)

    def remote(src, dst, send, recv, f2, i2):
        return pltpu.make_async_remote_copy(
            src_ref=src, dst_ref=dst, send_sem=send, recv_sem=recv,
            device_id={"ffn": f2, "emb": i2}, device_id_type=MESH,
        )

    def await_bytes(ref, sem):
        pltpu.make_async_copy(ref, ref, sem).wait()

    cols = pl.ds(pl.multiple_of(i * lw, 256), lw)

    def send_small(i2):
        remote(wr_ref, wr.at[i], s_send, s_recv.at[i], f, i2).start()
        remote(pre_ref, pre.at[cols], n_send.at[0], n_recv.at[0, i], f, i2).start()
        remote(post_ref, post.at[cols], n_send.at[1], n_recv.at[1, i], f, i2).start()

    own_h = pltpu.make_async_copy(h_ref.at[rows(c * half, half), :], hb.at[i], h_recv.at[i])
    own_h.start()
    pltpu.make_async_copy(wr_ref, wr.at[i], s_recv.at[i]).start()
    pltpu.make_async_copy(pre_ref, pre.at[cols], n_recv.at[0, i]).start()
    pltpu.make_async_copy(post_ref, post.at[cols], n_recv.at[1, i]).start()
    across = rows(f * (half // 2), half // 2)
    far = rows((1 - f) * (half // 2), half // 2)
    for c2 in range(2):
        i2 = 2 * (1 - x) + c2
        send_small(i2)
        src = h_ref.at[rows(c2 * half + f * (half // 2), half // 2), :]
        remote(src, hb.at[i, across, :], h_send.at[c2], h_recv.at[i], f, i2).start()
    send_small(sib)
    remote(h_ref.at[rows((1 - c) * half, half), :], hb.at[i], h_send.at[2], h_recv.at[i], f, sib).start()

    def blocks(j, fs, es):
        return (
            w0.at[j, fs, rows(es * lw, lw), :],
            w1.at[j, fs, rows(es * lw, lw), :],
            w2.at[j, es, rows(fs * fw, fw), :],
        )

    def group(j):
        return w0.at[j, 0, pl.ds(0, 3 * lw), :]

    mine = pl.ds(local_e * q, local_e)
    own_blocks = (
        w0.at[:, f, rows(i * lw, lw), :],
        w1.at[:, f, rows(i * lw, lw), :],
        w2.at[:, i, rows(f * fw, fw), :],
    )
    for src, to in zip((wg_ref.at[mine], wu_ref.at[mine], wd_ref.at[mine]), own_blocks):
        pltpu.make_async_copy(src, to, w_own).start()
        remote(src, to, f_send.at[0], f_own, f, sib).start()

    def send_block(j, m, d):
        x2, f2, q2 = chip(d)
        src = (wg_ref, wu_ref, wd_ref)[m].at[local_e * q2 + j]
        remote(src, blocks(j, f, i)[m], w_send.at[d - 1], w_recv.at[j, d - 1], f2, 2 * x2 + c).start()

    def send_expert(j, skip=0):
        for m in range(3):
            for d in (3 - c, 2 + c) + (() if m < skip else (1,)):
                send_block(j, m, d)

    ahead, begun = 3, 2
    for j in range(2):
        send_expert(j)
    for m in range(begun):
        send_block(2, m, 1)

    await_bytes(choice_ref, c_sem)

    sublane = lax.broadcasted_iota(jnp.int32, (experts, tile), 0)

    def chosen(start):
        ch = choice_ref[:, pl.ds(pl.multiple_of(start, LANES), tile)]
        a = jnp.zeros((experts, tile), f32)
        for k in range(choice_ref.shape[0]):
            a = a + jnp.where(ch[k : k + 1, :] == sublane, 1.0, 0.0)
        return a

    def count(n, total):
        return total + jnp.sum(chosen(n * tile), axis=1, keepdims=True)

    first = lax.fori_loop(0, half // tile, count, jnp.zeros((experts, 1), f32))
    strict = lax.broadcasted_iota(jnp.int32, (tile, tile), 0) < lax.broadcasted_iota(jnp.int32, (tile, tile), 1)
    strict = jnp.where(strict, 1.0, 0.0).astype(bf16)

    def place(n, carry):
        a = chosen(c * half + n * tile)
        before = carry + jnp.dot(a.astype(bf16), strict, preferred_element_type=f32)
        gates[rows(n * tile, tile), :] = jnp.where(before < capacity, a, 0.0).T
        for b in range(4):
            acc[b, rows(n * tile, tile), :] = jnp.zeros((tile, lw), f32)
        return carry + jnp.sum(a, axis=1, keepdims=True)

    lax.fori_loop(0, half // tile, place, first * c.astype(f32))

    for c2 in range(2):
        e2 = 2 * (1 - x) + c2
        await_bytes(hb.at[e2, across, :], h_recv.at[e2])
        ref = hb.at[e2, across, :]
        remote(ref, ref, hf_send.at[c2], hf_recv.at[c2], 1 - f, i).start()
    for j in range(2, ahead):
        send_expert(j, begun if j == 2 else 0)
    for c2 in range(2):
        await_bytes(hb.at[2 * x + c2], h_recv.at[2 * x + c2])
        await_bytes(hb.at[2 * (1 - x) + c2, far, :], hf_recv.at[c2])
    for b in range(4):
        await_bytes(wr.at[b], s_recv.at[b])
        for n, ref in enumerate((pre, post)):
            await_bytes(ref.at[pl.ds(b * lw, lw)], n_recv.at[n, b])

    def forward(j):
        for d in (1, 3, 2):
            x2, f2, _q2 = chip(d)
            await_bytes(group(j), w_recv.at[j, d - 1])
            for ref in blocks(j, f2, 2 * x2 + c):
                remote(ref, ref, f_send.at[d], f_recv.at[j], f, sib).start()

    forward(0)

    def route(n, _):
        r = rows(n * tile, tile)
        sq = jnp.zeros((tile, 1), f32)
        for b in range(4):
            hv = hb[b, r, :].astype(f32)
            sq = sq + jnp.sum(hv * hv, axis=1, keepdims=True)
        inv = lax.rsqrt(sq / (4 * lw) + EPS)
        logits = jnp.zeros((tile, experts), f32)
        for b in range(4):
            normed = (hb[b, r, :].astype(f32) * inv * pre[b * lw : (b + 1) * lw].astype(f32)[None, :]).astype(bf16)
            xn[r, b * lw : (b + 1) * lw] = normed
            logits = logits + lax.dot_general(
                normed, wr[b], (((1,), (1,)), ((), ())), preferred_element_type=f32
            )
        p = jnp.exp(logits - jnp.max(logits, axis=1, keepdims=True))
        p = p / jnp.sum(p, axis=1, keepdims=True)
        gates[r, :] = jnp.where(gates[r, :] > 0.0, p, 0.0)
        return 0

    lax.fori_loop(0, half // tile, route, 0)

    def piece(xs, fs, t):
        return acc.at[2 * xs + t % 2, rows(fs * 2 * quarter + t // 2 * part, part), :]

    def landing(slot, t):
        return rbuf.at[slot, t % 2, rows(t // 2 * part, part), :]

    def along_x(src, slot, t):
        return remote(src, landing(slot, t), r_send.at[slot], r_recv.at[slot, t], f, 2 * (1 - x) + c)

    def along_y(src, slot, t):
        return remote(src, landing(slot, t), r_send.at[slot], r_recv.at[slot, t], 1 - f, i)

    sent = w0.at[pl.ds(0, 3 * local_e // 8)]
    await_bytes(sent, w_own)
    await_bytes(sent, f_own)

    lane_q = lax.broadcasted_iota(jnp.int32, (quarter, experts), 1)

    def expert(j, last):
        if not last:
            @pl.when(j + ahead < local_e)
            def _():
                send_expert(j + ahead)

        if last:
            forward(j)
        else:
            @pl.when(j >= 1)
            def _():
                forward(j)

        await_bytes(xn.at[pl.ds(0, 9 * lw * fw // xn.shape[1]), :], f_recv.at[j])

        count = 8 if last else 4
        size = half // count

        def step(n, _):
            r = rows((((1 - f) * count // 2 + n) % count) * size, size)
            gate = jnp.sum(jnp.where(lane_q[0:size] == local_e * q + j, gates[r, :], 0.0), axis=1, keepdims=True)
            for s in range(2):
                z0 = jnp.dot(xn[r, :], w0[j, s], preferred_element_type=f32).astype(bf16).astype(f32)
                z1 = jnp.dot(xn[r, :], w1[j, s], preferred_element_type=f32).astype(bf16).astype(f32)
                g = jnp.where(gate > 0.0, gelu_tanh(z0) * z1, 0.0)
                gb[0:size, s * fw : (s + 1) * fw] = g.astype(bf16)
            for b in range(4):
                y = jnp.dot(gb[0:size, :], w2[j, b], preferred_element_type=f32).astype(bf16).astype(f32)
                u = (y * gate).astype(bf16).astype(f32)
                acc[b, r, :] += u

            if last:
                for k in range(count):
                    starts = [p for p in FIRST if p[2] == k]
                    if starts:
                        @pl.when(n == k)
                        def _():
                            for kind, t, _k in starts:
                                start_piece(kind, t)

            return 0

        lax.fori_loop(0, count, step, 0)

    def start_piece(kind, t):
        along_first, along_last = (along_y, along_x) if t in Y_FIRST else (along_x, along_y)
        near = (x, 1 - f) if t in Y_FIRST else (1 - x, f)
        if kind == "D":
            along_first(piece(1 - x, 1 - f, t), 0, t).start()
        elif kind == "N":
            along_first(piece(*near, t), 1, t).start()
        else:
            far = (1 - x, f) if t in Y_FIRST else (x, 1 - f)
            along_last(piece(*far, t), 2, t).start()

    def experts_but_last(j, _):
        expert(j, False)
        return 0

    lax.fori_loop(0, local_e - 1, experts_but_last, 0)
    expert(local_e - 1, True)

    def add_to(xs, fs, t):
        here = piece(xs, fs, t)
        await_bytes(landing(0, t), r_recv.at[0, t])
        here[...] = here[...] + landing(0, t)[...]

    def total(t):
        r = rows(f * 2 * quarter + t * part, part)
        s = rows(t * part, part)
        sq = jnp.zeros((part, part), f32)
        for b in range(2):
            for slot in (1, 2):
                await_bytes(landing(slot, 2 * t + b), r_recv.at[slot, 2 * t + b])
            v = acc[2 * x + b, r, :] + (rbuf[1, b, s, :] + rbuf[2, b, s, :])
            acc[2 * x + b, r, :] = v
            v = v * v
            sq = sq + (v[:, 0:128] + v[:, 128:256])
        sq_own[t] = jnp.broadcast_to(jnp.sum(sq.T, axis=0, keepdims=True), (8, part))
        remote(sq_own.at[t], sq_far.at[t], q_send, q_recv.at[t], f, 2 * (1 - x) + c).start()

    def out_rows(fs, cs, t):
        return out_ref.at[rows(cs * half + fs * 2 * quarter + t * part, part), :]

    def emit(t):
        r = rows(f * 2 * quarter + t * part, part)
        s = rows(t * part, part)
        await_bytes(sq_far.at[t], q_recv.at[t])
        inv = lax.rsqrt((sq_own[t, 0:1, :] + sq_far[t, 0:1, :]) / (4 * lw) + EPS)
        inv = jnp.broadcast_to(inv, (part, part)).T
        for b in range(2):
            gain = post[pl.ds(pl.multiple_of((2 * x + b) * lw, 256), lw)].astype(f32)[None, :]
            for g in range(lw // part):
                cols = slice(g * part, (g + 1) * part)
                m = acc[2 * x + b, r, cols]
                hv = hb[2 * x + b, r, cols].astype(f32)
                ob[b, s, cols] = (hv + m * inv * gain[:, cols]).astype(bf16)
        for b in range(2):
            remote(
                ob.at[b, s, :], out_rows(f, c, t), o_send.at[b], o_recv.at[c], 1 - f, 2 * x + b
            ).start()
        own = rows(c * half + f * 2 * quarter + t * part, part)
        out_ref[own, :] = ob[c, s, :]
        remote(ob.at[1 - c, s, :], out_rows(f, c, t), o_send.at[2], o_recv.at[2], f, sib).start()

    for kind, t in REST:
        if kind == "m":
            add_to(*((1 - x, f) if t in Y_FIRST else (x, 1 - f)), t)
        elif kind == "t":
            total(t)
        elif kind == "e":
            emit(t)
        else:
            start_piece(kind, t)

    for n in range(3):
        await_bytes(ob.at[0], o_recv.at[n])
        await_bytes(ob.at[0], o_send.at[n])
        await_bytes(rbuf.at[0], r_send.at[n])
    await_bytes(sq_own, q_send)

    await_bytes(wr.at[pl.ds(0, 3)], s_send)
    for n in range(2):
        await_bytes(pre.at[pl.ds(0, 3 * lw)], n_send.at[n])
    await_bytes(hb.at[0], h_send.at[2])
    for n in range(2):
        await_bytes(hb.at[0, across, :], h_send.at[n])
        await_bytes(hb.at[0, across, :], hf_send.at[n])

    for d in range(4):
        await_bytes(sent, f_send.at[d])
        if d:
            await_bytes(sent, w_send.at[d - 1])


def solution(mesh):
    emb_size = mesh.shape["emb"]
    ffn_size = mesh.shape["ffn"]
    assert emb_size == 4 and ffn_size == 2

    def local_block(hidden, norm_pre, norm_post, w_router, w_gate, w_up, w_down, choice):
        num_tok, lw = hidden.shape
        experts, _, fw = w_gate.shape
        top_k = choice.shape[1]
        capacity = 2 * num_tok * top_k // experts
        width, ffn = lw * emb_size, fw * ffn_size
        half, quarter, local_e = num_tok // 2, num_tok // 8, experts // 4
        parts = 2 * quarter // 128
        bf16, f32 = jnp.bfloat16, jnp.float32
        dma = pltpu.SemaphoreType.DMA
        anywhere = pl.BlockSpec(memory_space=pl.ANY)
        flops = 2 * 3 * half * local_e * width * ffn
        return pl.pallas_call(
            functools.partial(kernel, experts, capacity),
            out_shape=pltpu.VMEM((num_tok, lw), bf16),
            in_specs=[anywhere] * 8,
            out_specs=pl.BlockSpec(memory_space=pltpu.VMEM),
            scratch_shapes=[
                pltpu.VMEM((top_k, num_tok), jnp.int32),
                pltpu.VMEM((4, half, lw), bf16),
                pltpu.VMEM((4, experts, lw), bf16),
                pltpu.VMEM((width,), bf16),
                pltpu.VMEM((width,), bf16),
                pltpu.VMEM((local_e, 2, width, fw), bf16),
                pltpu.VMEM((local_e, 2, width, fw), bf16),
                pltpu.VMEM((local_e, 4, ffn, lw), bf16),
                pltpu.VMEM((half, width), bf16),
                pltpu.VMEM((half, experts), f32),
                pltpu.VMEM((4, half, lw), f32),
                pltpu.VMEM((3, 2, 2 * quarter, lw), f32),
                pltpu.VMEM((parts, 8, 128), f32),
                pltpu.VMEM((parts, 8, 128), f32),
                pltpu.VMEM((2, 2 * quarter, lw), bf16),
                pltpu.VMEM((quarter, ffn), bf16),
                dma((3,)), dma((4,)), dma((2,)), dma((2,)), dma(()), dma((4,)), dma((2,)), dma((2, 4)), dma(()),
                dma((3,)), dma((local_e, 3)), dma(()), dma(()),
                dma((4,)), dma((local_e,)),
                dma((3,)), dma((3, 2 * parts)), dma(()), dma((parts,)),
                dma((3,)), dma((3,)),
            ],
            compiler_params=pltpu.CompilerParams(
                collective_id=0, has_side_effects=True, vmem_limit_bytes=58 << 20
            ),
            cost_estimate=pl.CostEstimate(flops=flops, bytes_accessed=60 << 20, transcendentals=half * local_e * ffn),
        )(hidden, w_gate, w_up, w_down, w_router.T, norm_pre, norm_post, choice.T)

    in_specs = (P('dp', 'emb'), P('emb'), P('emb'), P('emb', None), P(None, 'emb', 'ffn'), P(None, 'emb', 'ffn'), P(None, 'ffn', 'emb'), P('dp', None))
    return jax.shard_map(local_block, mesh=mesh, in_specs=in_specs, out_specs=P('dp', 'emb'), check_vma=False)
```

```python
import functools
import math

import jax
import jax.numpy as jnp
from jax import lax
from jax.experimental import pallas as pl
from jax.experimental.pallas import tpu as pltpu
from jax.sharding import PartitionSpec as P

EPS = 1e-5
LANES = 128
MESH = pl.DeviceIdType.MESH


PIECES = 16
Y_FIRST = (2, 6, 8, 10, 13)
ORDER = (
    "D3", "D0", "D1", "D2", "N2", "N6", "D5", "N13", "N5", "D6", "m2", "m3", "m0", "D7", "N10", "m1",
    "N0", "M3", "m5", "D4", "D10", "m6", "M6", "M1", "m7", "N1", "M0", "N11", "D13", "m4", "m10", "N3",
    "M4", "M2", "D8", "t0", "M7", "m13", "N4", "N8", "D12", "M5", "D9", "m8", "t1", "e0", "M8", "m12",
    "M12", "N9", "N7", "t2", "m9", "M9", "e1", "D11", "M10", "D15", "t4", "t3", "e2", "m11", "M11", "N12",
    "M13", "D14", "m15", "M15", "e3", "t5", "e4", "N14", "t6", "N15", "m14", "M14", "e5", "e6", "t7", "e7",
)


def plan():
    steps = [(p[0], int(p[1:])) for p in ORDER]
    head = next(n for n, p in enumerate(steps) if p[0] == "m")
    first, tile = [], 0
    for kind, t in steps[:head]:
        need = t // 4 + (4 if kind == "N" and t not in Y_FIRST else 0)
        tile = max(tile, need)
        first.append((kind, t, tile))
    return first, steps[head:]


FIRST, REST = plan()


def gelu_tanh(z):
    return z * (0.5 * (1.0 + jnp.tanh(math.sqrt(2.0 / math.pi) * (z + 0.044715 * (z * z * z)))))


def kernel(
    experts, capacity,
    h_ref, wg_ref, wu_ref, wd_ref, wr_ref, pre_ref, post_ref, choice_hbm, out_ref,
    choice_ref, hb, wr, pre, post, w0, w1, w2, xn, gates, acc, rbuf, sq_own, sq_far, ob, gb,
    h_send, h_recv, hf_send, hf_recv, s_send, s_recv, n_send, n_recv, c_sem, w_send, w_recv, w_own, f_own, f_send, f_recv,
    r_send, r_recv, m_recv, q_send, q_recv, o_send, o_recv,
):
    num_tok, lw = h_ref.shape
    fw = wg_ref.shape[2]
    half = num_tok // 2
    quarter = num_tok // 8
    local_e = experts // 4
    tile = 256
    part = 128
    parts = quarter * 2 // part
    bf16, f32 = jnp.bfloat16, jnp.float32

    f = lax.axis_index("ffn")
    i = lax.axis_index("emb")
    x, c = i // 2, i % 2
    q = 2 * x + f
    sib = 2 * x + (1 - c)

    def chip(d):
        x2 = (x + d // 2) % 2
        f2 = (f + d % 2) % 2
        return x2, f2, 2 * x2 + f2

    def rows(start, size):
        return pl.ds(pl.multiple_of(start, 128), size)

    pltpu.make_async_copy(choice_hbm, choice_ref, c_sem).start()

    barrier = pltpu.get_barrier_semaphore()
    for f2, i2 in (
        (1 - f, 2 * (1 - x) + c), (1 - f, 2 * (1 - x) + 1 - c), (1 - f, i), (1 - f, sib),
        (f, 2 * (1 - x) + c), (f, 2 * (1 - x) + 1 - c), (f, sib),
    ):
        pl.semaphore_signal(barrier, inc=1, device_id={"ffn": f2, "emb": i2}, device_id_type=MESH)
    pl.semaphore_wait(barrier, 7)

    def remote(src, dst, send, recv, f2, i2):
        return pltpu.make_async_remote_copy(
            src_ref=src, dst_ref=dst, send_sem=send, recv_sem=recv,
            device_id={"ffn": f2, "emb": i2}, device_id_type=MESH,
        )

    def await_bytes(ref, sem):
        pltpu.make_async_copy(ref, ref, sem).wait()

    cols = pl.ds(pl.multiple_of(i * lw, 256), lw)

    def send_small(i2):
        remote(wr_ref, wr.at[i], s_send, s_recv.at[i], f, i2).start()
        remote(pre_ref, pre.at[cols], n_send.at[0], n_recv.at[0, i], f, i2).start()
        remote(post_ref, post.at[cols], n_send.at[1], n_recv.at[1, i], f, i2).start()

    own_h = pltpu.make_async_copy(h_ref.at[rows(c * half, half), :], hb.at[i], h_recv.at[i])
    own_h.start()
    pltpu.make_async_copy(wr_ref, wr.at[i], s_recv.at[i]).start()
    pltpu.make_async_copy(pre_ref, pre.at[cols], n_recv.at[0, i]).start()
    pltpu.make_async_copy(post_ref, post.at[cols], n_recv.at[1, i]).start()
    across = rows(f * (half // 2), half // 2)
    far = rows((1 - f) * (half // 2), half // 2)
    for c2 in range(2):
        i2 = 2 * (1 - x) + c2
        send_small(i2)
        src = h_ref.at[rows(c2 * half + f * (half // 2), half // 2), :]
        remote(src, hb.at[i, across, :], h_send.at[c2], h_recv.at[i], f, i2).start()
    send_small(sib)
    remote(h_ref.at[rows((1 - c) * half, half), :], hb.at[i], h_send.at[2], h_recv.at[i], f, sib).start()

    def blocks(j, fs, es):
        return (
            w0.at[j, fs, rows(es * lw, lw), :],
            w1.at[j, fs, rows(es * lw, lw), :],
            w2.at[j, es, rows(fs * fw, fw), :],
        )

    def group(j):
        return w0.at[j, 0, pl.ds(0, 3 * lw), :]

    mine = pl.ds(local_e * q, local_e)
    own_blocks = (
        w0.at[:, f, rows(i * lw, lw), :],
        w1.at[:, f, rows(i * lw, lw), :],
        w2.at[:, i, rows(f * fw, fw), :],
    )
    for src, to in zip((wg_ref.at[mine], wu_ref.at[mine], wd_ref.at[mine]), own_blocks):
        pltpu.make_async_copy(src, to, w_own).start()
        remote(src, to, f_send.at[0], f_own, f, sib).start()

    def send_block(j, m, d):
        x2, f2, q2 = chip(d)
        src = (wg_ref, wu_ref, wd_ref)[m].at[local_e * q2 + j]
        remote(src, blocks(j, f, i)[m], w_send.at[d - 1], w_recv.at[j, d - 1], f2, 2 * x2 + c).start()

    def send_expert(j, skip=0):
        for m in range(3):
            for d in (3 - c, 2 + c) + (() if m < skip else (1,)):
                send_block(j, m, d)

    ahead, begun = 3, 2
    for j in range(2):
        send_expert(j)
    for m in range(begun):
        send_block(2, m, 1)

    await_bytes(choice_ref, c_sem)

    sublane = lax.broadcasted_iota(jnp.int32, (experts, tile), 0)

    def chosen(start):
        ch = choice_ref[:, pl.ds(pl.multiple_of(start, LANES), tile)]
        a = jnp.zeros((experts, tile), f32)
        for k in range(choice_ref.shape[0]):
            a = a + jnp.where(ch[k : k + 1, :] == sublane, 1.0, 0.0)
        return a

    def count(n, total):
        return total + jnp.sum(chosen(n * tile), axis=1, keepdims=True)

    first = lax.fori_loop(0, half // tile, count, jnp.zeros((experts, 1), f32))
    strict = lax.broadcasted_iota(jnp.int32, (tile, tile), 0) < lax.broadcasted_iota(jnp.int32, (tile, tile), 1)
    strict = jnp.where(strict, 1.0, 0.0).astype(bf16)

    def place(n, carry):
        a = chosen(c * half + n * tile)
        before = carry + jnp.dot(a.astype(bf16), strict, preferred_element_type=f32)
        gates[rows(n * tile, tile), :] = jnp.where(before < capacity, a, 0.0).T
        for b in range(4):
            acc[b, rows(n * tile, tile), :] = jnp.zeros((tile, lw), f32)
        return carry + jnp.sum(a, axis=1, keepdims=True)

    lax.fori_loop(0, half // tile, place, first * c.astype(f32))

    for c2 in range(2):
        e2 = 2 * (1 - x) + c2
        await_bytes(hb.at[e2, across, :], h_recv.at[e2])
        ref = hb.at[e2, across, :]
        remote(ref, ref, hf_send.at[c2], hf_recv.at[c2], 1 - f, i).start()
    for j in range(2, ahead):
        send_expert(j, begun if j == 2 else 0)
    for c2 in range(2):
        await_bytes(hb.at[2 * x + c2], h_recv.at[2 * x + c2])
        await_bytes(hb.at[2 * (1 - x) + c2, far, :], hf_recv.at[c2])
    for b in range(4):
        await_bytes(wr.at[b], s_recv.at[b])
        for n, ref in enumerate((pre, post)):
            await_bytes(ref.at[pl.ds(b * lw, lw)], n_recv.at[n, b])

    def forward(j):
        for d in (1, 3, 2):
            x2, f2, _q2 = chip(d)
            await_bytes(group(j), w_recv.at[j, d - 1])
            for ref in blocks(j, f2, 2 * x2 + c):
                remote(ref, ref, f_send.at[d], f_recv.at[j], f, sib).start()

    forward(0)

    def route(n, _):
        r = rows(n * tile, tile)
        sq = jnp.zeros((tile, 1), f32)
        for b in range(4):
            hv = hb[b, r, :].astype(f32)
            sq = sq + jnp.sum(hv * hv, axis=1, keepdims=True)
        inv = lax.rsqrt(sq / (4 * lw) + EPS)
        logits = jnp.zeros((tile, experts), f32)
        for b in range(4):
            normed = (hb[b, r, :].astype(f32) * inv * pre[b * lw : (b + 1) * lw].astype(f32)[None, :]).astype(bf16)
            xn[r, b * lw : (b + 1) * lw] = normed
            logits = logits + lax.dot_general(
                normed, wr[b], (((1,), (1,)), ((), ())), preferred_element_type=f32
            )
        p = jnp.exp(logits - jnp.max(logits, axis=1, keepdims=True))
        p = p / jnp.sum(p, axis=1, keepdims=True)
        gates[r, :] = jnp.where(gates[r, :] > 0.0, p, 0.0)
        return 0

    lax.fori_loop(0, half // tile, route, 0)

    def piece(xs, fs, t):
        return acc.at[2 * xs + t % 2, rows(fs * 2 * quarter + t // 2 * part, part), :]

    def landing(slot, t):
        return rbuf.at[slot, t % 2, rows(t // 2 * part, part), :]

    def arrival(slot, t):
        return m_recv.at[t // 2] if slot else r_recv.at[t]

    def along_x(src, slot, t):
        return remote(src, landing(slot, t), r_send.at[slot], arrival(slot, t), f, 2 * (1 - x) + c)

    def along_y(src, slot, t):
        return remote(src, landing(slot, t), r_send.at[slot], arrival(slot, t), 1 - f, i)

    sent = w0.at[pl.ds(0, 3 * local_e // 8)]
    await_bytes(sent, w_own)
    await_bytes(sent, f_own)

    lane_q = lax.broadcasted_iota(jnp.int32, (quarter, experts), 1)

    def expert(j, last):
        if not last:
            @pl.when(j + ahead < local_e)
            def _():
                send_expert(j + ahead)

        if last:
            forward(j)
        else:
            @pl.when(j >= 1)
            def _():
                forward(j)

        await_bytes(xn.at[pl.ds(0, 9 * lw * fw // xn.shape[1]), :], f_recv.at[j])

        count = 8 if last else 4
        size = half // count

        def step(n, _):
            r = rows((((1 - f) * count // 2 + n) % count) * size, size)
            gate = jnp.sum(jnp.where(lane_q[0:size] == local_e * q + j, gates[r, :], 0.0), axis=1, keepdims=True)
            for s in range(2):
                z0 = jnp.dot(xn[r, :], w0[j, s], preferred_element_type=f32).astype(bf16).astype(f32)
                z1 = jnp.dot(xn[r, :], w1[j, s], preferred_element_type=f32).astype(bf16).astype(f32)
                g = jnp.where(gate > 0.0, gelu_tanh(z0) * z1, 0.0)
                gb[0:size, s * fw : (s + 1) * fw] = g.astype(bf16)
            for b in range(4):
                y = jnp.dot(gb[0:size, :], w2[j, b], preferred_element_type=f32).astype(bf16).astype(f32)
                u = (y * gate).astype(bf16).astype(f32)
                acc[b, r, :] += u

            if last:
                for k in range(count):
                    starts = [p for p in FIRST if p[2] == k]
                    if starts:
                        @pl.when(n == k)
                        def _():
                            for kind, t, _k in starts:
                                start_piece(kind, t)

            return 0

        lax.fori_loop(0, count, step, 0)

    def start_piece(kind, t):
        along_first, along_last = (along_y, along_x) if t in Y_FIRST else (along_x, along_y)
        near = (x, 1 - f) if t in Y_FIRST else (1 - x, f)
        if kind == "D":
            along_first(piece(1 - x, 1 - f, t), 0, t).start()
        elif kind == "N":
            along_first(piece(*near, t), 1, t).start()
        else:
            far = (1 - x, f) if t in Y_FIRST else (x, 1 - f)
            along_last(piece(*far, t), 2, t).start()

    def experts_but_last(j, _):
        expert(j, False)
        return 0

    lax.fori_loop(0, local_e - 1, experts_but_last, 0)
    expert(local_e - 1, True)

    def add_to(xs, fs, t):
        here = piece(xs, fs, t)
        await_bytes(landing(0, t), r_recv.at[t])
        here[...] = here[...] + landing(0, t)[...]

    def total(t):
        r = rows(f * 2 * quarter + t * part, part)
        s = rows(t * part, part)
        await_bytes(ob.at[0], m_recv.at[t])
        sq = jnp.zeros((part, part), f32)
        for b in range(2):
            v = acc[2 * x + b, r, :] + (rbuf[1, b, s, :] + rbuf[2, b, s, :])
            acc[2 * x + b, r, :] = v
            v = v * v
            sq = sq + (v[:, 0:128] + v[:, 128:256])
        sq_own[t] = jnp.broadcast_to(jnp.sum(sq.T, axis=0, keepdims=True), (8, part))
        remote(sq_own.at[t], sq_far.at[t], q_send, q_recv.at[t], f, 2 * (1 - x) + c).start()

    def out_rows(fs, cs, t):
        return out_ref.at[rows(cs * half + fs * 2 * quarter + t * part, part), :]

    def emit(t):
        r = rows(f * 2 * quarter + t * part, part)
        s = rows(t * part, part)
        await_bytes(sq_far.at[t], q_recv.at[t])
        inv = lax.rsqrt((sq_own[t, 0:1, :] + sq_far[t, 0:1, :]) / (4 * lw) + EPS)
        inv = jnp.broadcast_to(inv, (part, part)).T
        for b in range(2):
            gain = post[pl.ds(pl.multiple_of((2 * x + b) * lw, 256), lw)].astype(f32)[None, :]
            for g in range(lw // part):
                cols = slice(g * part, (g + 1) * part)
                m = acc[2 * x + b, r, cols]
                hv = hb[2 * x + b, r, cols].astype(f32)
                ob[b, s, cols] = (hv + m * inv * gain[:, cols]).astype(bf16)
        for b in range(2):
            remote(
                ob.at[b, s, :], out_rows(f, c, t), o_send.at[b], o_recv.at[c], 1 - f, 2 * x + b
            ).start()
        own = rows(c * half + f * 2 * quarter + t * part, part)
        out_ref[own, :] = ob[c, s, :]
        remote(ob.at[1 - c, s, :], out_rows(f, c, t), o_send.at[2], o_recv.at[2], f, sib).start()

    for kind, t in REST:
        if kind == "m":
            add_to(*((1 - x, f) if t in Y_FIRST else (x, 1 - f)), t)
        elif kind == "t":
            total(t)
        elif kind == "e":
            emit(t)
        else:
            start_piece(kind, t)

    for n in range(3):
        await_bytes(ob.at[0], o_recv.at[n])
        await_bytes(ob.at[0], o_send.at[n])
        await_bytes(rbuf.at[0], r_send.at[n])
    await_bytes(sq_own, q_send)

    await_bytes(wr.at[pl.ds(0, 3)], s_send)
    for n in range(2):
        await_bytes(pre.at[pl.ds(0, 3 * lw)], n_send.at[n])
    await_bytes(hb.at[0], h_send.at[2])
    for n in range(2):
        await_bytes(hb.at[0, across, :], h_send.at[n])
        await_bytes(hb.at[0, across, :], hf_send.at[n])

    for d in range(4):
        await_bytes(sent, f_send.at[d])
        if d:
            await_bytes(sent, w_send.at[d - 1])


def solution(mesh):
    emb_size = mesh.shape["emb"]
    ffn_size = mesh.shape["ffn"]
    assert emb_size == 4 and ffn_size == 2

    def local_block(hidden, norm_pre, norm_post, w_router, w_gate, w_up, w_down, choice):
        num_tok, lw = hidden.shape
        experts, _, fw = w_gate.shape
        top_k = choice.shape[1]
        capacity = 2 * num_tok * top_k // experts
        width, ffn = lw * emb_size, fw * ffn_size
        half, quarter, local_e = num_tok // 2, num_tok // 8, experts // 4
        parts = 2 * quarter // 128
        bf16, f32 = jnp.bfloat16, jnp.float32
        dma = pltpu.SemaphoreType.DMA
        anywhere = pl.BlockSpec(memory_space=pl.ANY)
        flops = 2 * 3 * half * local_e * width * ffn
        return pl.pallas_call(
            functools.partial(kernel, experts, capacity),
            out_shape=pltpu.VMEM((num_tok, lw), bf16),
            in_specs=[anywhere] * 8,
            out_specs=pl.BlockSpec(memory_space=pltpu.VMEM),
            scratch_shapes=[
                pltpu.VMEM((top_k, num_tok), jnp.int32),
                pltpu.VMEM((4, half, lw), bf16),
                pltpu.VMEM((4, experts, lw), bf16),
                pltpu.VMEM((width,), bf16),
                pltpu.VMEM((width,), bf16),
                pltpu.VMEM((local_e, 2, width, fw), bf16),
                pltpu.VMEM((local_e, 2, width, fw), bf16),
                pltpu.VMEM((local_e, 4, ffn, lw), bf16),
                pltpu.VMEM((half, width), bf16),
                pltpu.VMEM((half, experts), f32),
                pltpu.VMEM((4, half, lw), f32),
                pltpu.VMEM((3, 2, 2 * quarter, lw), f32),
                pltpu.VMEM((parts, 8, 128), f32),
                pltpu.VMEM((parts, 8, 128), f32),
                pltpu.VMEM((2, 2 * quarter, lw), bf16),
                pltpu.VMEM((quarter, ffn), bf16),
                dma((3,)), dma((4,)), dma((2,)), dma((2,)), dma(()), dma((4,)), dma((2,)), dma((2, 4)), dma(()),
                dma((3,)), dma((local_e, 3)), dma(()), dma(()),
                dma((4,)), dma((local_e,)),
                dma((3,)), dma((2 * parts,)), dma((parts,)), dma(()), dma((parts,)),
                dma((3,)), dma((3,)),
            ],
            compiler_params=pltpu.CompilerParams(
                collective_id=0, has_side_effects=True, vmem_limit_bytes=58 << 20
            ),
            cost_estimate=pl.CostEstimate(flops=flops, bytes_accessed=60 << 20, transcendentals=half * local_e * ffn),
        )(hidden, w_gate, w_up, w_down, w_router.T, norm_pre, norm_post, choice.T)

    in_specs = (P('dp', 'emb'), P('emb'), P('emb'), P('emb', None), P(None, 'emb', 'ffn'), P(None, 'emb', 'ffn'), P(None, 'ffn', 'emb'), P('dp', None))
    return jax.shard_map(local_block, mesh=mesh, in_specs=in_specs, out_specs=P('dp', 'emb'), check_vma=False)
```
